512 devices in a mesh: chan: 16 (over x, y_lo), slab: 32 (over z, y_hi, core).
Axes of the slice: x: 4, y: 8 (y_hi: 2, y_lo: 4; y = y_hi * 4 + y_lo), z: 8, core: 2. Of those that a mesh axis runs over, the one named last changes fastest.
Arguments:
- taylor_models: float32 [2, 2048, 2048], P(None, 'slab', 'chan'), may hold values from -6 to 6
- gridded_vis: bfloat16 [16, 2, 2048, 2048], P('chan', None, 'slab'), may hold values from -6 to 6
- uv_weight: bfloat16 [16, 2048, 2048], P('chan', 'slab'), may hold values from 0 to 2
- freq_ratio: float32 [16], P('chan'), may hold values from 0.6 to 1.4
- robust_scale: float32 [16], P('chan'), may hold values from 0.25 to 4
Outputs:
- taylor_residual: float32 [2, 2048, 2048], P(None, 'slab', 'chan')
The draws below stay inside these ranges and needn't reach their ends.
All inputs are finite; a program needn't handle non-finite values.
Results may differ from the reference program's by a relative error of at most 0.0003.
Values sent between devices are 32-bit elements; how exact they have to be, the bound alone decides.
A program may use at most 64 MiB of HBM per device.

```python
import math
import jax
import jax.numpy as jnp
from jax import lax

PIX = 2048
TERMS = 2
CHANNELS = 16


def levels(key, dims, cuts, smallest, largest):
    factor_of = 1.0
    for position, parts in cuts:
        steps = jax.random.uniform(jax.random.fold_in(jax.random.fold_in(key, 6), position), (parts,), jnp.float32, smallest / len(cuts), largest / len(cuts))
        factor_of = factor_of * jnp.repeat(jnp.exp(steps), dims[position] // parts).reshape((-1,) + (1,) * (len(dims) - 1 - position))
    return factor_of


def centred(own_key, extent, deviation, bound, pieces=(), dtype=jnp.bfloat16):
    entries = deviation * jax.random.normal(own_key, extent, jnp.float32)
    if pieces:
        entries = entries * levels(own_key, extent, pieces, -0.22, 0.18)
    return jnp.clip(entries, -bound, bound).astype(dtype)


def setup_inputs(seed: int = 0) -> dict:
    keys = jax.random.split(jax.random.key(seed), 6)
    taylor_models = centred(keys[0], (TERMS, PIX, PIX), 1.0, 6.0, ((1, 32), (2, 16)), jnp.float32)
    gridded_vis = centred(keys[1], (CHANNELS, 2, PIX, PIX), 1.0, 6.0, ((0, 16), (2, 32)))
    uv_weight = jnp.clip(2.0 * jax.random.uniform(keys[2], (CHANNELS, PIX, PIX), jnp.float32) ** levels(keys[2], (CHANNELS, PIX, PIX), ((0, 16), (1, 32)), -0.2, 0.2), 0.0, 2.0).astype(jnp.bfloat16)
    freq_ratio = jnp.clip(0.6 + 0.79999995 * jax.random.uniform(keys[3], (CHANNELS,), jnp.float32) ** levels(keys[3], (CHANNELS,), ((0, 16),), -0.2, 0.2), 0.6, 1.4)
    robust_scale = jnp.clip(jnp.exp(math.log(4.0) - 2.7725887 * jax.random.uniform(keys[4], (CHANNELS,), jnp.float32) ** levels(keys[4], (CHANNELS,), ((0, 16),), -0.2, 0.2)), 0.25, 4.0)
    return {"taylor_models": taylor_models, "gridded_vis": gridded_vis, "uv_weight": uv_weight, "freq_ratio": freq_ratio, "robust_scale": robust_scale}


def reference(taylor_models, gridded_vis, uv_weight, freq_ratio, robust_scale):
    def one_channel(carry, item):
        visible, weight, ratio, damping = item
        offset = ratio - 1.0
        sky_image = taylor_models[0]
        for term_index in range(1, TERMS):
            sky_image = sky_image + offset ** term_index * taylor_models[term_index]
        spectrum = jnp.fft.fft2(sky_image, norm="ortho").T
        visible_wide = visible.astype(jnp.float32)
        weight_wide = weight.astype(jnp.float32)
        delta_real = visible_wide[0] - weight_wide * jnp.real(spectrum)
        delta_imag = visible_wide[1] - weight_wide * jnp.imag(spectrum)
        robust = 1.0 / (1.0 + damping * (delta_real * delta_real + delta_imag * delta_imag))
        weighted = lax.complex(robust * delta_real, robust * delta_imag)
        residual = jnp.real(jnp.fft.ifft2(weighted.T, norm="ortho"))
        layers = [residual]
        for term_index in range(1, TERMS):
            layers.append(offset ** term_index * residual)
        return carry + jnp.stack(layers), None

    initial = jnp.zeros((TERMS, PIX, PIX), jnp.float32)
    total, _ = lax.scan(one_channel, initial, (gridded_vis, uv_weight, freq_ratio, robust_scale))
    return total
```

```python
import functools

import jax
import jax.numpy as jnp
import numpy as np
from jax import lax
from jax.experimental import pallas as pl
from jax.experimental.pallas import tpu as pltpu
from jax.sharding import PartitionSpec as P

PIX = 2048
F32, BF16 = jnp.float32, jnp.bfloat16
MESH = pl.DeviceIdType.MESH
NC, NS, NX = 16, 32, 4


def rep(angle):
    c, s = np.cos(angle), np.sin(angle)
    return np.array([[c, s], [-s, c]])


def tables():
    tau = 2 * np.pi
    j, c = np.arange(16), np.arange(16)
    ang = tau * np.outer(j, c) / 16
    first = np.stack([np.cos(ang), -np.sin(ang)])
    t_a = np.einsum("ijc,rq->ijrcq", first, np.eye(8)).reshape(256, 128)
    ang = np.repeat(tau * np.outer(j, np.arange(128)) / PIX, 8, axis=0)
    w_a = np.stack([np.cos(ang), -np.sin(ang)])
    b = rep(tau * np.outer(np.arange(128), np.arange(128)) / 128)
    t_b = np.einsum("oika->koia", b).reshape(256, 256)
    y1 = 8 * np.arange(32)[None, :] + np.arange(8)[:, None]
    d = rep(tau * (np.arange(256)[:, None, None] * y1 % 256) / 256)
    t_d = np.einsum("oipgs->opgis", d).reshape(512, 512)
    ang = np.tile(tau * np.outer(np.arange(256), np.arange(8)) / PIX, (1, 16))
    w_d = np.stack([np.cos(ang), -np.sin(ang)]) / PIX
    e = rep(tau * np.outer(np.arange(8), np.arange(8)) / 8)
    t_e = np.einsum("oimr,jq->omjiqr", e, np.eye(16)).reshape(256, 256)
    return [x.astype(np.float32) for x in (t_a, w_a, t_b, t_d, w_d, t_e)]


def split(x):
    hi = x.astype(BF16)
    return hi, (x - hi.astype(F32)).astype(BF16)


def dot3(a, b, nt):
    dims = (((1,), (1 if nt else 0,)), ((), ()))

    def one(p, q):
        return lax.dot_general(p, q, dims, preferred_element_type=F32)

    return one(a[0], b[0]) + one(a[0], b[1]) + one(a[1], b[0])


def both(ref):
    return ref[0], ref[1]


def kernel(
    freq, robust, taylor, vis, wt, t_a, w_a, t_b, t_d, w_d, t_e, out,
    tay_v, vis_v, wt_v, va, vwa, vb, vd, vwd, ve,
    ma, mat, mb, md, mdt, me2, met, vwdt,
    buf1, snd2, buf2, snd3, buf3, fs, ws, snd5, buf5, snd6, buf6, snd7, buf7,
    vsend, vrecv, prm,
    lsem, s1, s2, s3, s5, s6, s7, sv, sp, r1, r2, r3, r5, r6, r7, rv, rp,
):
    chan, slab = lax.axis_index("chan"), lax.axis_index("slab")
    mx, my = chan // 4, chan % 4

    loads = [
        pltpu.make_async_copy(src, dst, lsem.at[i])
        for i, (src, dst) in enumerate(
            [(taylor, tay_v), (vis, vis_v), (wt, wt_v), (t_a, va), (w_a, vwa),
             (t_b, vb), (t_d, vd), (w_d, vwd), (t_e, ve)]
        )
    ]
    for cp in loads:
        cp.start()

    barrier = pltpu.get_barrier_semaphore()

    def greet_slab(d, _):
        pl.semaphore_signal(barrier, inc=1, device_id={"slab": (slab + d) % NS}, device_id_type=MESH)
        return 0

    def greet_chan(d, _):
        pl.semaphore_signal(barrier, inc=1, device_id={"chan": (chan + d) % NC}, device_id_type=MESH)
        return 0

    lax.fori_loop(1, NS, greet_slab, 0)
    lax.fori_loop(1, NC, greet_chan, 0)

    rows = lax.broadcasted_iota(jnp.int32, (8, 128), 0)
    prm[pl.ds(mx, 1)] = jnp.where(rows == 0, freq[0] - 1.0, robust[0])[None]
    loads[1].wait()
    loads[2].wait()
    for q in range(NX):
        for p in range(2):
            vsend[q, p] = vis_v[p, 16 * q : 16 * q + 16].astype(F32)
        vsend[q, 2] = wt_v[16 * q : 16 * q + 16].astype(F32)
    loads[0].wait()

    pl.semaphore_wait(barrier, NS + NC - 2)

    def tile(ref, i, n=8):
        return ref.at[pl.ds(pl.multiple_of(i * n, n), n)]

    def to_chan(src, dst, n, send, recv, d):
        peer = (chan + d) % NC
        return pltpu.make_async_remote_copy(
            tile(src, peer, n), tile(dst, chan, n), send.at[d], recv,
            device_id={"chan": peer}, device_id_type=MESH)

    def to_slab(src, dst, send, recv, d):
        peer = (slab + d) % NS
        return pltpu.make_async_remote_copy(
            tile(src, peer), tile(dst, slab), send.at[d], recv,
            device_id={"slab": peer}, device_id_type=MESH)

    def go(make, n):
        def step(d, _):
            make(d).start()
            return 0
        lax.fori_loop(1, n, step, 0)

    def sent(make, n):
        def step(d, _):
            make(d).wait_send()
            return 0
        lax.fori_loop(1, n, step, 0)

    def landed(buf, sem):
        pltpu.make_async_copy(buf, buf, sem).wait()

    x1 = functools.partial(to_chan, tay_v, buf1, 8, s1, r1)
    go(x1, NC)
    pltpu.make_async_copy(tile(tay_v, chan), tile(buf1, chan), r1).start()

    def xp(d):
        return pltpu.make_async_remote_copy(
            prm.at[mx], prm.at[mx], sp.at[d], rp.at[d],
            device_id={"chan": (mx + d) % NX * 4 + my}, device_id_type=MESH)

    def xv(d):
        peer = (mx + d) % NX
        return pltpu.make_async_remote_copy(
            vsend.at[peer], vrecv.at[d - 1], sv.at[d], rv.at[d],
            device_id={"chan": peer * 4 + my}, device_id_type=MESH)

    for d in (1, 3, 2):
        xp(d).start()
    for d in (1, 3, 2):
        xv(d).start()

    def put(dst, x):
        dst[0], dst[1] = split(x)

    for i in (3, 4, 5):
        loads[i].wait()
    put(ma, va[...])
    put(mb, vb[...])

    landed(buf1, r1)
    pre = dot3(both(ma), split(buf1[...]), False)
    re, im = pre[:128], pre[128:]
    yre = re * vwa[0] - im * vwa[1]
    yim = re * vwa[1] + im * vwa[0]
    snd2[...] = dot3(both(mb), split(jnp.concatenate([yre, yim], axis=1)), True)

    x2 = functools.partial(to_slab, snd2, buf2, s2, r2)
    go(x2, NS)
    pltpu.make_async_copy(tile(snd2, slab), tile(buf2, slab), r2).start()

    for i in (6, 7, 8):
        loads[i].wait()
    put(md, vd[...])
    put(me2, ve[...])
    put(mat, va[...].T)
    put(met, ve[...].T)
    put(mdt, vd[...].T)
    vwdt[0] = vwd[0].T
    vwdt[1] = vwd[1].T

    landed(buf2, r2)
    for q in range(4):
        for p in range(2):
            snd3[pl.ds(64 * q + 32 * p, 32)] = buf2[pl.ds(2 * q + p, 32, stride=8)]

    def x3(d):
        peer = (chan + d) % NC
        return pltpu.make_async_remote_copy(
            tile(snd3, peer // 4, 64), tile(buf3, chan, 64), s3.at[d], r3,
            device_id={"chan": peer}, device_id_type=MESH)

    go(x3, NC)
    pltpu.make_async_copy(tile(snd3, mx, 64), tile(buf3, chan, 64), r3).start()
    landed(buf3, r3)

    x = jnp.concatenate([buf3[:512], buf3[512:]], axis=1)
    pre = dot3(both(md), split(x), False)
    parts = []
    for t in range(2):
        re, im = pre[:256, 128 * t : 128 * t + 128], pre[256:, 128 * t : 128 * t + 128]
        parts.append(jnp.concatenate(
            [re * vwd[0] - im * vwd[1], re * vwd[1] + im * vwd[0]], axis=1))
    fs[...] = dot3(both(me2), split(jnp.concatenate(parts, axis=0)), True)

    for d in (1, 3, 2):
        xp(d).wait_recv()
        xv(d).wait_recv()

    def point(m, _):
        lo, hi = pl.ds(pl.multiple_of(16 * m, 16), 16), pl.ds(pl.multiple_of(128 + 16 * m, 16), 16)
        lane = pl.ds(pl.multiple_of(256 * m, 256), 256)
        f0r, f1r = fs[lo, :256], fs[lo, 256:]
        f0i, f1i = fs[hi, :256], fs[hi, 256:]
        sums = [jnp.zeros((16, 256), F32)] * 4
        for d in range(NX):
            who = (mx - d + NX) % NX
            pair = prm[pl.ds(who, 1)][0]
            off, damp = pair[0:1, 0:1], pair[1:2, 0:1]
            if d == 0:
                vr, vi, w = (vsend[pl.ds(mx, 1), p, :, lane][0] for p in range(3))
            else:
                vr, vi, w = (vrecv[d - 1, p, :, lane] for p in range(3))
            dr = vr - w * (f0r + off * f1r)
            di = vi - w * (f0i + off * f1i)
            k = 1.0 / (1.0 + damp * (dr * dr + di * di))
            wr, wi = k * dr, k * di
            sums = [sums[0] + wr, sums[1] + wi, sums[2] + off * wr, sums[3] + off * wi]
        ws[lo, :256], ws[hi, :256], ws[lo, 256:], ws[hi, 256:] = sums
        return 0

    lax.fori_loop(0, 8, point, 0)

    pre = dot3(both(met), split(ws[...]), False)
    parts = []
    for t in range(2):
        re, im = pre[:128, 256 * t : 256 * t + 256], pre[128:, 256 * t : 256 * t + 256]
        parts.append(jnp.concatenate(
            [re * vwdt[0] + im * vwdt[1], im * vwdt[0] - re * vwdt[1]], axis=1))
    back = dot3(both(mdt), split(jnp.concatenate(parts, axis=0)), True)
    snd5[:512] = back[:, :128]
    snd5[512:] = back[:, 128:]

    x5 = functools.partial(to_chan, snd5, buf5, 64, s5, r5)
    go(x5, NC)
    pltpu.make_async_copy(tile(snd5, chan, 64), tile(buf5, chan, 64), r5).start()
    landed(buf5, r5)
    for q in range(4):
        b = 256 * q
        acc = (buf5[b : b + 64] + buf5[b + 64 : b + 128]) + (buf5[b + 128 : b + 192] + buf5[b + 192 : b + 256])
        for p in range(2):
            snd6[pl.ds(2 * q + p, 32, stride=8)] = acc[32 * p : 32 * p + 32]

    x6 = functools.partial(to_slab, snd6, buf6, s6, r6)
    go(x6, NS)
    pltpu.make_async_copy(tile(snd6, slab), tile(buf6, slab), r6).start()
    landed(buf6, r6)
    z = dot3(split(buf6[...].T), both(mb), False)
    re, im = z[:, :128], z[:, 128:]
    z = jnp.concatenate([re * vwa[0] + im * vwa[1], im * vwa[0] - re * vwa[1]], axis=0)
    snd7[...] = dot3(both(mat), split(z), False)

    x7 = functools.partial(to_chan, snd7, buf7, 8, s7, r7)
    go(x7, NC)
    pltpu.make_async_copy(tile(snd7, chan), tile(buf7, chan), r7).start()

    sent(x1, NC)
    sent(x2, NS)
    sent(x3, NC)
    sent(x5, NC)
    sent(x6, NS)
    for d in (1, 3, 2):
        xp(d).wait_send()
        xv(d).wait_send()
    sent(x7, NC)
    landed(buf7, r7)
    out[...] = buf7[...]


def local(taylor_models, gridded_vis, uv_weight, freq_ratio, robust_scale):
    tabs = [jnp.asarray(x) for x in tables()]
    any_space = pl.BlockSpec(memory_space=pl.ANY)
    smem = pl.BlockSpec(memory_space=pltpu.SMEM)
    v = pltpu.VMEM
    dma = pltpu.SemaphoreType.DMA
    scratch = (
        [v((128, 128), F32), v((2, 64, PIX), BF16), v((64, PIX), BF16)]
        + [v(x.shape, F32) for x in tabs]
        + [v((2, *s), BF16) for s in
           ((256, 128), (128, 256), (256, 256), (512, 512), (512, 512), (256, 256), (256, 256))]
        + [v((2, 128, 256), F32)]
        + [v((n, m), F32) for n, m in
           ((128, 128), (256, 128), (256, 128), (256, 128), (1024, 128), (256, 512), (256, 512),
            (1024, 128), (1024, 128), (256, 128), (256, 128), (128, 128), (128, 128))]
        + [v((4, 3, 16, PIX), F32), v((3, 3, 16, PIX), F32), v((4, 8, 128), F32)]
        + [dma((9,)), dma((NC,)), dma((NS,)), dma((NC,)), dma((NC,)), dma((NS,)), dma((NC,)),
           dma((4,)), dma((4,))]
        + [dma, dma, dma, dma, dma, dma, dma((4,)), dma((4,))]
    )
    out = pl.pallas_call(
        kernel,
        out_shape=jax.ShapeDtypeStruct((128, 128), F32),
        in_specs=[smem, smem] + [any_space] * 9,
        out_specs=pl.BlockSpec(memory_space=pltpu.VMEM),
        scratch_shapes=scratch,
        compiler_params=pltpu.CompilerParams(
            collective_id=0, has_side_effects=True, vmem_limit_bytes=40 * 1024 * 1024),
    )(freq_ratio, robust_scale, taylor_models.reshape(128, 128), gridded_vis[0], uv_weight[0], *tabs)
    return out.reshape(2, 64, 128)


def solution(mesh):
    placed = (
        P(None, "slab", "chan"),
        P("chan", None, "slab", None),
        P("chan", "slab", None),
        P("chan"),
        P("chan"),
    )
    return jax.shard_map(
        local, mesh=mesh, in_specs=placed, out_specs=P(None, "slab", "chan"), check_vma=False
    )
```

```python
import functools

import jax
import jax.numpy as jnp
import numpy as np
from jax import lax
from jax.experimental import pallas as pl
from jax.experimental.pallas import tpu as pltpu
from jax.sharding import PartitionSpec as P

PIX = 2048
F32, BF16 = jnp.float32, jnp.bfloat16
MESH = pl.DeviceIdType.MESH
NC, NZ, NY = 16, 16, 32


EARLY, LATE = (2, 6, 1, 3, 7), (4, 5)


def rep(angle):
    c, s = np.cos(angle), np.sin(angle)
    return np.array([[c, s], [-s, c]])


def tables():
    tau = 2 * np.pi
    j, c = np.arange(16), np.arange(16)
    ang = tau * np.outer(j, c) / 16
    first = np.stack([np.cos(ang), -np.sin(ang)])
    t_a = np.einsum("ijc,rq->ijrcq", first, np.eye(8)).reshape(256, 128)
    ang = np.repeat(tau * np.outer(j, np.arange(128)) / PIX, 8, axis=0)
    w_a = np.stack([np.cos(ang), -np.sin(ang)])
    z, k, h, q = np.meshgrid(*map(np.arange, (8, 2, 2, 4)), indexing="ij")
    step = (((z * 2 + h) * 2 + k) * 4 + q).reshape(128)
    t_b = np.einsum("oika->okia", rep(tau * np.outer(step, np.arange(128)) / 128)).reshape(256, 256)
    h, g, z, k = np.meshgrid(*map(np.arange, (2, 8, 8, 2)), indexing="ij")
    y1 = (8 * ((z * 2 + h) * 2 + k) + g).reshape(256)
    ang = tau * (np.outer(np.arange(256), y1) % 256) / 256
    t_d = np.concatenate([np.cos(ang), np.sin(ang)])
    ang = np.tile(tau * np.outer(np.arange(256), np.arange(8)) / PIX, (1, 8))
    w_d = np.stack([np.tile(np.cos(ang), (1, 2)), np.concatenate([np.sin(ang), -np.sin(ang)], axis=1)]) / PIX
    e = rep(tau * np.outer(np.arange(8), np.arange(8)) / 8)
    t_e = np.einsum("oimr,jq->omjiqr", e, np.eye(8)).reshape(128, 128)
    return [x.astype(np.float32) for x in (t_a, w_a, t_b, t_d, w_d, t_e)]


def split(x):
    hi = x.astype(BF16)
    return hi, (x - hi.astype(F32)).astype(BF16)


def dot3(a, b, nt):
    dims = (((1,), (1 if nt else 0,)), ((), ()))

    def one(p, q):
        return lax.dot_general(p, q, dims, preferred_element_type=F32)

    return one(a[0], b[0]) + one(a[0], b[1]) + one(a[1], b[0])


def both(ref):
    return ref[0], ref[1]


def swap(x):
    return pltpu.roll(x, 64, axis=1)


def kernel(
    freq, robust, taylor, vis, wt, t_a, w_a, t_b, t_d, w_d, t_e, out,
    freq_s, robust_s, tay_v, vis_v, wt_v, va, vwa, vb, vd, vwd, ve,
    ma, mat, mb, md, mdt, me2, met, vwdt,
    buf1, snd2, buf2, snd3, buf3, fs, ws, snd5, buf5, snd6, buf6, snd7, buf7,
    vsend, vrecv, prm,
    lsem, s1, s2, s3, s5, s6, s7, sv, sp, r1, r2, r3, r5, r6, r7, rv, rp,
):
    def turn(i, d, n):
        return lax.rem(i + d, n)

    chan, slab = lax.axis_index("chan"), lax.axis_index("slab")
    mx, my = lax.div(chan, 4), lax.rem(chan, 4)
    mp, me = lax.div(my, 2), lax.rem(my, 2)
    mk, mh, z = lax.rem(slab, 2), lax.rem(lax.div(slab, 2), 2), lax.div(slab, 4)
    mz = z * 2 + mk
    mo = mx * 2 + me
    xs, ys = [turn(mx, d, 4) for d in range(4)], [turn(my, d, 4) for d in range(4)]
    hs, ks = [mh, 1 - mh], [mk, 1 - mk]
    es = [lax.rem(y, 2) for y in ys]
    x_rows = [lax.div(x, 2) * 16 + lax.rem(x, 2) * 4 for x in xs]
    slab_h = [slab, slab + 2 - 4 * mh]
    FAR = (2, 3, 1, 0)

    chan_peers = [
        (xs[i] * 4 + ys[j], {"chan": xs[i] * 4 + ys[j]}) for i in FAR for j in FAR if i or j]
    y_peers = [
        (hs[h] * 8 + xs[i] * 2 + es[j], x_rows[i] + hs[h] * 8 + ys[j],
         {"chan": xs[i] * 4 + ys[j], "slab": slab_h[h]})
        for h in (1, 0) for i in FAR for j in FAR if h or i or j]
    z_peers = []
    for d in (4, 3, 5, 2, 6, 1, 7, 0):
        for k in (1, 0):
            if d or k:
                far = turn(z, d, 8)
                z_peers.append((far * 2 + ks[k], {"slab": far * 4 + mh * 2 + ks[k]}))
    my_row, my_u = x_rows[0] + mh * 8 + my, mh * 8 + mo

    barrier = pltpu.get_barrier_semaphore()
    for peer in y_peers + z_peers:
        pl.semaphore_signal(barrier, inc=1, device_id=peer[-1], device_id_type=MESH)

    loads = [
        pltpu.make_async_copy(src, dst, lsem.at[i])
        for i, (src, dst) in enumerate(
            [(taylor, tay_v), (vis, vis_v), (wt, wt_v), (t_a, va), (w_a, vwa),
             (t_b, vb), (t_d, vd), (w_d, vwd), (t_e, ve), (freq, freq_s), (robust, robust_s)]
        )
    ]
    for i in (9, 10, 0, 1, 2, 3, 4, 5, 6, 7, 8):
        loads[i].start()

    rows = lax.broadcasted_iota(jnp.int32, (8, 128), 0)
    loads[9].wait()
    loads[10].wait()
    prm[pl.ds(mo, 1)] = jnp.where(rows == 0, freq_s[0] - 1.0, robust_s[0])[None]
    loads[1].wait()
    loads[2].wait()
    for q in range(4):
        for p in range(3):
            src = wt_v[16 * q : 16 * q + 16] if p == 2 else vis_v[p, 16 * q : 16 * q + 16]
            wide = src.astype(F32)
            vsend[2 * q, p] = wide[:8]
            vsend[2 * q + 1, p] = wide[8:]
    loads[0].wait()

    pl.semaphore_wait(barrier, len(y_peers) + len(z_peers))

    def tile(ref, i, n=8):
        return ref.at[pl.ds(pl.multiple_of(i * n, n), n)]

    def spread(peers, src, dst, mine, kept, n, send, recv, which=0):
        for peer in peers:
            pltpu.make_async_remote_copy(
                tile(src, peer[which], n), tile(dst, mine, n), send, recv,
                device_id=peer[-1], device_id_type=MESH).start()
        pltpu.make_async_copy(tile(src, kept, n), tile(dst, mine, n), recv).start()

    def landed(buf, sem):
        pltpu.make_async_copy(buf, buf, sem).wait()

    spread(chan_peers, tay_v, buf1, chan, chan, 8, s1, r1)

    def ally(d):
        x, e = xs[d // 2], es[d % 2]
        return x * 2 + e, {"chan": x * 4 + mp * 2 + e}

    def xp(d):
        return pltpu.make_async_remote_copy(
            prm.at[mo], prm.at[mo], sp, rp.at[d], device_id=ally(d)[1], device_id_type=MESH)

    def xv(d):
        o, device = ally(d)
        return pltpu.make_async_remote_copy(
            vsend.at[o], vrecv.at[d - 1], sv, rv.at[d], device_id=device, device_id_type=MESH)

    for d in EARLY + LATE:
        xp(d).start()
    for d in EARLY:
        xv(d).start()

    def put(dst, x):
        dst[0], dst[1] = split(x)

    for i in (3, 4, 5):
        loads[i].wait()
    put(ma, va[...])
    put(mb, vb[...])

    landed(buf1, r1)
    low = lax.broadcasted_iota(jnp.int32, (128, 128), 1) < 64
    pre = dot3(both(ma), split(buf1[...]), False)
    re, im = pre[:128], pre[128:]
    yre = re * vwa[0] - im * vwa[1]
    yim = re * vwa[1] + im * vwa[0]
    pre = dot3(both(mb), split(jnp.concatenate([yre, yim], axis=1)), True)
    re, im = pre[:128], pre[128:]
    snd2[pl.ds(0, 128, stride=2)] = jnp.where(low, re, swap(im))
    snd2[pl.ds(1, 128, stride=2)] = jnp.where(low, swap(re), im)

    spread(z_peers, snd2, buf2, mz, mz, 16, s2, r2)

    for i in (6, 7, 8):
        loads[i].wait()
    put(md, vd[...])
    put(me2, ve[...])
    put(mat, va[...].T)
    put(met, ve[...].T)
    put(mdt, jnp.concatenate([vd[:256].T, vd[256:].T], axis=0))
    vwdt[0] = vwd[0, :, :].T
    vwdt[1] = vwd[1, :, :].T

    landed(buf2, r2)
    for i in range(16):
        snd3[16 * i : 16 * i + 16] = buf2[pl.ds(i, 16, stride=16)]

    spread(y_peers, snd3, buf3, my_row, my_u, 16, s3, r3)
    for d in LATE:
        xv(d).start()
    landed(buf3, r3)

    x = jnp.concatenate([buf3[:256], buf3[256:]], axis=1)
    pre = dot3(both(md), split(x), False)
    sign = jnp.where(lax.broadcasted_iota(jnp.int32, (256, 128), 1) < 64, 1.0, -1.0)
    parts = []
    for t in range(2):
        lanes = slice(128 * t, 128 * t + 128)
        y = pre[:256, lanes] + sign * swap(pre[256:, lanes])
        parts.append(y * vwd[0] + swap(y) * vwd[1])
    fs[...] = dot3(both(me2), split(jnp.concatenate(parts, axis=0)), True)

    def point(first, group, m, _):
        lo, hi = pl.ds(pl.multiple_of(8 * m, 8), 8), pl.ds(pl.multiple_of(64 + 8 * m, 8), 8)
        lane = pl.ds(pl.multiple_of(256 * m, 256), 256)
        f0r, f1r = fs[lo, :256], fs[lo, 256:]
        f0i, f1i = fs[hi, :256], fs[hi, 256:]
        if first:
            sums = [jnp.zeros((8, 256), F32)] * 4
        else:
            sums = [ws[lo, :256], ws[hi, :256], ws[lo, 256:], ws[hi, 256:]]
        for d in group:
            who = turn(mx, 4 - d // 2, 4) * 2 + es[d % 2]
            pair = prm[pl.ds(who, 1)][0]
            off, damp = pair[0:1, 0:1], pair[1:2, 0:1]
            if d == 0:
                vr, vi, w = (vsend[pl.ds(mo, 1), p, :, lane][0] for p in range(3))
            else:
                vr, vi, w = (vrecv[d - 1, p, :, lane] for p in range(3))
            dr = vr - w * (f0r + off * f1r)
            di = vi - w * (f0i + off * f1i)
            k = 1.0 / (1.0 + damp * (dr * dr + di * di))
            wr, wi = k * dr, k * di
            sums = [sums[0] + wr, sums[1] + wi, sums[2] + off * wr, sums[3] + off * wi]
        ws[lo, :256], ws[hi, :256], ws[lo, 256:], ws[hi, 256:] = sums
        return 0

    for d in EARLY:
        xp(d).wait_recv()
        xv(d).wait_recv()
    lax.fori_loop(0, 8, functools.partial(point, True, (0,) + EARLY), 0)
    for d in LATE:
        xp(d).wait_recv()
        xv(d).wait_recv()
    lax.fori_loop(0, 8, functools.partial(point, False, LATE), 0)

    pre = dot3(both(met), split(ws[...]), False)
    parts = []
    for t in range(2):
        re, im = pre[:64, 256 * t : 256 * t + 256], pre[64:, 256 * t : 256 * t + 256]
        parts += [re * vwdt[0, :64] - im * vwdt[1, :64], im * vwdt[0, :64] + re * vwdt[1, :64]]
    back = dot3(both(mdt), split(jnp.concatenate(parts, axis=0)), True)
    for t in range(2):
        lanes = slice(128 * t, 128 * t + 128)
        snd5[256 * t : 256 * t + 256] = back[:256, lanes] - sign * swap(back[256:, lanes])

    spread(y_peers, snd5, buf5, mp * 16 + my_u, my_row, 16, s5, r5, 1)
    landed(buf5, r5)
    for i in range(16):
        b = 16 * i
        snd6[pl.ds(i, 16, stride=16)] = buf5[b : b + 16] + buf5[256 + b : 272 + b]

    spread(z_peers, snd6, buf6, mz, mz, 16, s6, r6)
    landed(buf1.at[: 8 * (NC - 1)], s1)
    landed(buf2.at[: 16 * (NZ - 1)], s2)
    landed(buf3.at[: 16 * (NY - 1)], s3)
    landed(buf5.at[: 16 * (NY - 1)], s5)
    landed(prm.at[:7], sp)
    landed(vrecv, sv)
    landed(buf6, r6)
    p0, p1 = buf6[pl.ds(0, 128, stride=2)], buf6[pl.ds(1, 128, stride=2)]
    re, im = jnp.where(low, p0, swap(p1)), jnp.where(low, swap(p0), p1)
    z = dot3(split(jnp.concatenate([re.T, im.T], axis=1)), both(mb), False)
    re, im = z[:, :128], z[:, 128:]
    z = jnp.concatenate([re * vwa[0] + im * vwa[1], im * vwa[0] - re * vwa[1]], axis=0)
    snd7[...] = dot3(both(mat), split(z), False)

    spread(chan_peers, snd7, buf7, chan, chan, 8, s7, r7)
    landed(buf7, r7)
    landed(buf6.at[: 16 * (NZ - 1)], s6)
    landed(buf7.at[: 8 * (NC - 1)], s7)
    out[...] = buf7[...]


def local(taylor_models, gridded_vis, uv_weight, freq_ratio, robust_scale):
    tabs = [jnp.asarray(x) for x in tables()]
    any_space = pl.BlockSpec(memory_space=pltpu.HBM)
    v = pltpu.VMEM
    dma = pltpu.SemaphoreType.DMA
    scratch = (
        [pltpu.SMEM((1,), F32), pltpu.SMEM((1,), F32), v((128, 128), F32), v((2, 64, PIX), BF16), v((64, PIX), BF16)]
        + [v(x.shape, F32) for x in tabs]
        + [v((2, *s), BF16) for s in
           ((256, 128), (128, 256), (256, 256), (512, 256), (512, 256), (128, 128), (128, 128))]
        + [v((2, 128, 256), F32)]
        + [v((n, m), F32) for n, m in
           ((128, 128), (256, 128), (256, 128), (256, 128), (512, 128), (128, 512), (128, 512),
            (512, 128), (512, 128), (256, 128), (256, 128), (128, 128), (128, 128))]
        + [v((8, 3, 8, PIX), F32), v((7, 3, 8, PIX), F32), v((8, 8, 128), F32)]
        + [dma((11,))] + [dma] * 8 + [dma] * 6 + [dma((8,)), dma((8,))]
    )
    out = pl.pallas_call(
        kernel,
        out_shape=jax.ShapeDtypeStruct((128, 128), F32),
        in_specs=[any_space] * 11,
        out_specs=pl.BlockSpec(memory_space=pltpu.VMEM),
        scratch_shapes=scratch,
        compiler_params=pltpu.CompilerParams(
            collective_id=0, has_side_effects=True, vmem_limit_bytes=66_000_000),
    )(freq_ratio, robust_scale, taylor_models.reshape(128, 128), gridded_vis[0], uv_weight[0], *tabs)
    return out.reshape(2, 64, 128)


def solution(mesh):
    placed = (
        P(None, "slab", "chan"),
        P("chan", None, "slab", None),
        P("chan", "slab", None),
        P("chan"),
        P("chan"),
    )
    return jax.shard_map(
        local, mesh=mesh, in_specs=placed, out_specs=P(None, "slab", "chan"), check_vma=False
    )
```

```python
import functools

import jax
import jax.numpy as jnp
import numpy as np
from jax import lax
from jax.experimental import pallas as pl
from jax.experimental.pallas import tpu as pltpu
from jax.sharding import PartitionSpec as P

PIX = 2048
F32, BF16 = jnp.float32, jnp.bfloat16
MESH = pl.DeviceIdType.MESH
NC, NZ, NY = 16, 16, 32


EARLY, LATE, CUT = (1, 5, 4, 2, 6, 3), (7,), 1


def rep(angle):
    c, s = np.cos(angle), np.sin(angle)
    return np.array([[c, s], [-s, c]])


def tables():
    tau = 2 * np.pi
    j, c = np.arange(16), np.arange(16)
    ang = tau * np.outer(j, c) / 16
    first = np.stack([np.cos(ang), -np.sin(ang)])
    t_a = np.einsum("ijc,rq->ijrcq", first, np.eye(8)).reshape(256, 128)
    ang = np.repeat(tau * np.outer(j, np.arange(128)) / PIX, 8, axis=0)
    w_a = np.stack([np.cos(ang), -np.sin(ang)])
    z, k, h, q = np.meshgrid(*map(np.arange, (8, 2, 2, 4)), indexing="ij")
    step = (((z * 2 + h) * 2 + k) * 4 + q).reshape(128)
    t_b = np.einsum("oika->okia", rep(tau * np.outer(step, np.arange(128)) / 128)).reshape(256, 256)
    h, g, z, k = np.meshgrid(*map(np.arange, (2, 8, 8, 2)), indexing="ij")
    y1 = (8 * ((z * 2 + h) * 2 + k) + g).reshape(256)
    ang = tau * (np.outer(np.arange(256), y1) % 256) / 256
    t_d = np.concatenate([np.cos(ang), np.sin(ang)])
    ang = np.tile(tau * np.outer(np.arange(256), np.arange(8)) / PIX, (1, 8))
    w_d = np.stack([np.tile(np.cos(ang), (1, 2)), np.concatenate([np.sin(ang), -np.sin(ang)], axis=1)]) / PIX
    e = rep(tau * np.outer(np.arange(8), np.arange(8)) / 8)
    t_e = np.einsum("oimr,jq->omjiqr", e, np.eye(8)).reshape(128, 128)
    return [x.astype(np.float32) for x in (t_a, w_a, t_b, t_d, w_d, t_e)]


def split(x):
    hi = x.astype(BF16)
    return hi, (x - hi.astype(F32)).astype(BF16)


def dot3(a, b, nt):
    dims = (((1,), (1 if nt else 0,)), ((), ()))

    def one(p, q):
        return lax.dot_general(p, q, dims, preferred_element_type=F32)

    return one(a[0], b[0]) + one(a[0], b[1]) + one(a[1], b[0])


def both(ref):
    return ref[0], ref[1]


def swap(x):
    return pltpu.roll(x, 64, axis=1)


def kernel(
    freq, robust, taylor, vis, wt, t_a, w_a, t_b, t_d, w_d, t_e, out,
    freq_s, robust_s, tay_v, vis_v, wt_v, va, vwa, vb, vd, vwd, ve,
    ma, mat, mb, md, mdt, me2, met, vwdt,
    buf1, snd2, buf2, snd3, buf3, fs, ws, snd5, buf5, snd6, buf6, snd7, buf7,
    vsend, vrecv, prm,
    lsem, s1, s2, s3, s5, s6, s7, sv, sp, r1, r2, r3, r5, r6, r7, rv, rp,
):
    def turn(i, d, n):
        return lax.rem(i + d, n)

    chan, slab = lax.axis_index("chan"), lax.axis_index("slab")
    mx, my = lax.div(chan, 4), lax.rem(chan, 4)
    mp, me = lax.div(my, 2), lax.rem(my, 2)
    mk, mh, z = lax.rem(slab, 2), lax.rem(lax.div(slab, 2), 2), lax.div(slab, 4)
    mz = z * 2 + mk
    mo = mx * 2 + me
    xs, ys = [turn(mx, d, 4) for d in range(4)], [turn(my, d, 4) for d in range(4)]
    ks, es = [mk, 1 - mk], [me, 1 - me]
    ring = [turn(mh * 4 + my, d, 8) for d in range(8)]
    x_rows = [lax.div(x, 2) * 16 + lax.rem(x, 2) * 4 for x in xs]
    FAR = (2, 3, 1, 0)

    chan_peers = [
        (xs[i] * 4 + ys[j], {"chan": xs[i] * 4 + ys[j]}) for i in FAR for j in FAR if i or j]
    y_peers = []
    for j in (4, 3, 5, 2, 6, 1, 7, 0):
        half, y = lax.div(ring[j], 4), lax.rem(ring[j], 4)
        side, there = half * 8 + lax.rem(y, 2), slab + 2 * (half - mh)
        for i in FAR:
            if i or j:
                y_peers.append((side + xs[i] * 2, x_rows[i] + half * 8 + y,
                                {"chan": xs[i] * 4 + y, "slab": there}))
    z_peers = []
    for d in (4, 3, 5, 2, 6, 1, 7, 0):
        for k in (1, 0):
            if d or k:
                far = turn(z, d, 8)
                z_peers.append((far * 2 + ks[k], {"slab": far * 4 + mh * 2 + ks[k]}))
    my_row, my_u = x_rows[0] + mh * 8 + my, mh * 8 + mo

    barrier = pltpu.get_barrier_semaphore()
    for peer in y_peers + z_peers:
        pl.semaphore_signal(barrier, inc=1, device_id=peer[-1], device_id_type=MESH)

    loads = [
        pltpu.make_async_copy(src, dst, lsem.at[i])
        for i, (src, dst) in enumerate(
            [(taylor, tay_v), (vis, vis_v), (wt, wt_v), (t_a, va), (w_a, vwa),
             (t_b, vb), (t_d, vd), (w_d, vwd), (t_e, ve), (freq, freq_s), (robust, robust_s)]
        )
    ]
    for i in (9, 10, 0, 1, 2, 3, 4, 5, 6, 7, 8):
        loads[i].start()

    rows = lax.broadcasted_iota(jnp.int32, (8, 128), 0)
    loads[9].wait()
    loads[10].wait()
    prm[pl.ds(mo, 1)] = jnp.where(rows == 0, freq_s[0] - 1.0, robust_s[0])[None]
    loads[1].wait()
    loads[2].wait()
    for q in range(4):
        for p in range(3):
            src = wt_v[16 * q : 16 * q + 16] if p == 2 else vis_v[p, 16 * q : 16 * q + 16]
            wide = src.astype(F32)
            vsend[2 * q, p] = wide[:8]
            vsend[2 * q + 1, p] = wide[8:]
    loads[0].wait()

    pl.semaphore_wait(barrier, len(y_peers) + len(z_peers))

    def tile(ref, i, n=8):
        return ref.at[pl.ds(pl.multiple_of(i * n, n), n)]

    def spread(peers, src, dst, mine, kept, n, send, recv, which=0):
        for peer in peers:
            pltpu.make_async_remote_copy(
                tile(src, peer[which], n), tile(dst, mine, n), send, recv,
                device_id=peer[-1], device_id_type=MESH).start()
        pltpu.make_async_copy(tile(src, kept, n), tile(dst, mine, n), recv).start()

    def landed(buf, sem):
        pltpu.make_async_copy(buf, buf, sem).wait()

    spread(chan_peers, tay_v, buf1, chan, chan, 8, s1, r1)

    def ally(d):
        x, e = xs[d // 2], es[d % 2]
        return x * 2 + e, {"chan": x * 4 + mp * 2 + e}

    def xp(d):
        return pltpu.make_async_remote_copy(
            prm.at[mo], prm.at[mo], sp, rp.at[d], device_id=ally(d)[1], device_id_type=MESH)

    def xv(d, planes):
        o, device = ally(d)
        for p in planes:
            pltpu.make_async_remote_copy(
                vsend.at[o, p], vrecv.at[d - 1, p], sv, rv.at[d],
                device_id=device, device_id_type=MESH).start()

    def arrived(d):
        xp(d).wait_recv()
        landed(vrecv.at[d - 1], rv.at[d])

    for d in EARLY + LATE:
        xp(d).start()
    for d in EARLY:
        xv(d, range(3))
    for d in LATE:
        xv(d, range(CUT))

    def put(dst, x):
        dst[0], dst[1] = split(x)

    for i in (3, 4, 5):
        loads[i].wait()
    put(ma, va[...])
    put(mb, vb[...])

    landed(buf1, r1)
    low = lax.broadcasted_iota(jnp.int32, (128, 128), 1) < 64
    pre = dot3(both(ma), split(buf1[...]), False)
    re, im = pre[:128], pre[128:]
    yre = re * vwa[0] - im * vwa[1]
    yim = re * vwa[1] + im * vwa[0]
    pre = dot3(both(mb), split(jnp.concatenate([yre, yim], axis=1)), True)
    re, im = pre[:128], pre[128:]
    snd2[pl.ds(0, 128, stride=2)] = jnp.where(low, re, swap(im))
    snd2[pl.ds(1, 128, stride=2)] = jnp.where(low, swap(re), im)

    spread(z_peers, snd2, buf2, mz, mz, 16, s2, r2)

    for i in (6, 7, 8):
        loads[i].wait()
    put(md, vd[...])
    put(me2, ve[...])
    put(mat, va[...].T)
    put(met, ve[...].T)
    put(mdt, jnp.concatenate([vd[:256].T, vd[256:].T], axis=0))
    vwdt[0] = vwd[0, :, :].T
    vwdt[1] = vwd[1, :, :].T

    landed(buf2, r2)
    for i in range(16):
        snd3[16 * i : 16 * i + 16] = buf2[pl.ds(i, 16, stride=16)]

    spread(y_peers, snd3, buf3, my_row, my_u, 16, s3, r3)
    for d in LATE:
        xv(d, range(CUT, 3))
    landed(buf3, r3)

    x = jnp.concatenate([buf3[:256], buf3[256:]], axis=1)
    pre = dot3(both(md), split(x), False)
    sign = jnp.where(lax.broadcasted_iota(jnp.int32, (256, 128), 1) < 64, 1.0, -1.0)
    parts = []
    for t in range(2):
        lanes = slice(128 * t, 128 * t + 128)
        y = pre[:256, lanes] + sign * swap(pre[256:, lanes])
        parts.append(y * vwd[0] + swap(y) * vwd[1])
    fs[...] = dot3(both(me2), split(jnp.concatenate(parts, axis=0)), True)

    def point(first, group, m, _):
        lo, hi = pl.ds(pl.multiple_of(8 * m, 8), 8), pl.ds(pl.multiple_of(64 + 8 * m, 8), 8)
        lane = pl.ds(pl.multiple_of(256 * m, 256), 256)
        f0r, f1r = fs[lo, :256], fs[lo, 256:]
        f0i, f1i = fs[hi, :256], fs[hi, 256:]
        if first:
            sums = [jnp.zeros((8, 256), F32)] * 4
        else:
            sums = [ws[lo, :256], ws[hi, :256], ws[lo, 256:], ws[hi, 256:]]
        for d in group:
            who = turn(mx, 4 - d // 2, 4) * 2 + es[d % 2]
            pair = prm[pl.ds(who, 1)][0]
            off, damp = pair[0:1, 0:1], pair[1:2, 0:1]
            if d == 0:
                vr, vi, w = (vsend[pl.ds(mo, 1), p, :, lane][0] for p in range(3))
            else:
                vr, vi, w = (vrecv[d - 1, p, :, lane] for p in range(3))
            dr = vr - w * (f0r + off * f1r)
            di = vi - w * (f0i + off * f1i)
            k = 1.0 / (1.0 + damp * (dr * dr + di * di))
            wr, wi = k * dr, k * di
            sums = [sums[0] + wr, sums[1] + wi, sums[2] + off * wr, sums[3] + off * wi]
        ws[lo, :256], ws[hi, :256], ws[lo, 256:], ws[hi, 256:] = sums
        return 0

    for d in EARLY:
        arrived(d)
    lax.fori_loop(0, 8, functools.partial(point, True, (0,) + EARLY), 0)
    for d in LATE:
        arrived(d)
    lax.fori_loop(0, 8, functools.partial(point, False, LATE), 0)

    pre = dot3(both(met), split(ws[...]), False)
    parts = []
    for t in range(2):
        re, im = pre[:64, 256 * t : 256 * t + 256], pre[64:, 256 * t : 256 * t + 256]
        parts += [re * vwdt[0, :64] - im * vwdt[1, :64], im * vwdt[0, :64] + re * vwdt[1, :64]]
    back = dot3(both(mdt), split(jnp.concatenate(parts, axis=0)), True)
    for t in range(2):
        lanes = slice(128 * t, 128 * t + 128)
        snd5[256 * t : 256 * t + 256] = back[:256, lanes] - sign * swap(back[256:, lanes])

    spread(y_peers, snd5, buf5, mp * 16 + my_u, my_row, 16, s5, r5, 1)
    landed(buf5, r5)
    for i in range(16):
        b = 16 * i
        snd6[pl.ds(i, 16, stride=16)] = buf5[b : b + 16] + buf5[256 + b : 272 + b]

    spread(z_peers, snd6, buf6, mz, mz, 16, s6, r6)
    landed(buf1.at[: 8 * (NC - 1)], s1)
    landed(buf2.at[: 16 * (NZ - 1)], s2)
    landed(buf3.at[: 16 * (NY - 1)], s3)
    landed(buf5.at[: 16 * (NY - 1)], s5)
    landed(prm.at[:7], sp)
    landed(vrecv, sv)
    landed(buf6, r6)
    p0, p1 = buf6[pl.ds(0, 128, stride=2)], buf6[pl.ds(1, 128, stride=2)]
    re, im = jnp.where(low, p0, swap(p1)), jnp.where(low, swap(p0), p1)
    z = dot3(split(jnp.concatenate([re.T, im.T], axis=1)), both(mb), False)
    re, im = z[:, :128], z[:, 128:]
    z = jnp.concatenate([re * vwa[0] + im * vwa[1], im * vwa[0] - re * vwa[1]], axis=0)
    snd7[...] = dot3(both(mat), split(z), False)

    spread(chan_peers, snd7, buf7, chan, chan, 8, s7, r7)
    landed(buf7, r7)
    landed(buf6.at[: 16 * (NZ - 1)], s6)
    landed(buf7.at[: 8 * (NC - 1)], s7)
    out[...] = buf7[...]


def local(taylor_models, gridded_vis, uv_weight, freq_ratio, robust_scale):
    tabs = [jnp.asarray(x) for x in tables()]
    any_space = pl.BlockSpec(memory_space=pltpu.HBM)
    v = pltpu.VMEM
    dma = pltpu.SemaphoreType.DMA
    scratch = (
        [pltpu.SMEM((1,), F32), pltpu.SMEM((1,), F32), v((128, 128), F32), v((2, 64, PIX), BF16), v((64, PIX), BF16)]
        + [v(x.shape, F32) for x in tabs]
        + [v((2, *s), BF16) for s in
           ((256, 128), (128, 256), (256, 256), (512, 256), (512, 256), (128, 128), (128, 128))]
        + [v((2, 128, 256), F32)]
        + [v((n, m), F32) for n, m in
           ((128, 128), (256, 128), (256, 128), (256, 128), (512, 128), (128, 512), (128, 512),
            (512, 128), (512, 128), (256, 128), (256, 128), (128, 128), (128, 128))]
        + [v((8, 3, 8, PIX), F32), v((7, 3, 8, PIX), F32), v((8, 8, 128), F32)]
        + [dma((11,))] + [dma] * 8 + [dma] * 6 + [dma((8,)), dma((8,))]
    )
    out = pl.pallas_call(
        kernel,
        out_shape=pltpu.VMEM((128, 128), F32),
        in_specs=[any_space] * 11,
        out_specs=pl.BlockSpec(memory_space=pltpu.VMEM),
        scratch_shapes=scratch,
        compiler_params=pltpu.CompilerParams(
            collective_id=0, has_side_effects=True, vmem_limit_bytes=66_000_000),
    )(freq_ratio, robust_scale, taylor_models.reshape(128, 128), gridded_vis[0], uv_weight[0], *tabs)
    return out.reshape(2, 64, 128)


def solution(mesh):
    placed = (
        P(None, "slab", "chan"),
        P("chan", None, "slab", None),
        P("chan", "slab", None),
        P("chan"),
        P("chan"),
    )
    return jax.shard_map(
        local, mesh=mesh, in_specs=placed, out_specs=P(None, "slab", "chan"), check_vma=False
    )
```

```python
import functools

import jax
import jax.numpy as jnp
import numpy as np
from jax import lax
from jax.experimental import pallas as pl
from jax.experimental.pallas import tpu as pltpu
from jax.sharding import PartitionSpec as P

PIX = 2048
F32, BF16 = jnp.float32, jnp.bfloat16
MESH = pl.DeviceIdType.MESH
NC, NZ, NY = 16, 16, 32


THIRD = ((7, 1), (7, 2))
SECOND = tuple((d, p) for d in (1, 5, 4, 2, 6, 3, 7) for p in range(3) if (d, p) not in THIRD)
EARLY, LATE = (1, 5, 4, 2, 6, 3), (7,)


def rep(angle):
    c, s = np.cos(angle), np.sin(angle)
    return np.array([[c, s], [-s, c]])


def tables():
    tau = 2 * np.pi
    j, c = np.arange(16), np.arange(16)
    ang = tau * np.outer(j, c) / 16
    first = np.stack([np.cos(ang), -np.sin(ang)])
    t_a = np.einsum("ijc,rq->ijrcq", first, np.eye(8)).reshape(256, 128)
    ang = np.repeat(tau * np.outer(j, np.arange(128)) / PIX, 8, axis=0)
    w_a = np.stack([np.cos(ang), -np.sin(ang)])
    z, k, h, q = np.meshgrid(*map(np.arange, (8, 2, 2, 4)), indexing="ij")
    step = (((z * 2 + h) * 2 + k) * 4 + q).reshape(128)
    t_b = np.einsum("oika->okia", rep(tau * np.outer(step, np.arange(128)) / 128)).reshape(256, 256)
    h, g, z, k = np.meshgrid(*map(np.arange, (2, 8, 8, 2)), indexing="ij")
    y1 = (8 * ((z * 2 + h) * 2 + k) + g).reshape(256)
    ang = tau * (np.outer(np.arange(256), y1) % 256) / 256
    t_d = np.concatenate([np.cos(ang), np.sin(ang)])
    ang = np.tile(tau * np.outer(np.arange(256), np.arange(8)) / PIX, (1, 8))
    w_d = np.stack([np.tile(np.cos(ang), (1, 2)), np.concatenate([np.sin(ang), -np.sin(ang)], axis=1)]) / PIX
    e = rep(tau * np.outer(np.arange(8), np.arange(8)) / 8)
    t_e = np.einsum("oimr,jq->omjiqr", e, np.eye(8)).reshape(128, 128)
    return [x.astype(np.float32) for x in (t_a, w_a, t_b, t_d, w_d, t_e)]


def split(x):
    hi = x.astype(BF16)
    return hi, (x - hi.astype(F32)).astype(BF16)


def dot3(a, b, nt):
    dims = (((1,), (1 if nt else 0,)), ((), ()))

    def one(p, q):
        return lax.dot_general(p, q, dims, preferred_element_type=F32)

    return one(a[0], b[0]) + one(a[0], b[1]) + one(a[1], b[0])


def both(ref):
    return ref[0], ref[1]


def swap(x):
    return pltpu.roll(x, 64, axis=1)


def kernel(
    freq, robust, taylor, vis, wt, t_a, w_a, t_b, t_d, w_d, t_e, out,
    freq_s, robust_s, tay_v, vis_v, wt_v, va, vwa, vb, vd, vwd, ve,
    ma, mat, mb, md, mdt, me2, met, vwdt,
    buf1, snd2, buf2, snd3, buf3, fs, ws, snd5, buf5, snd6, buf6, snd7, buf7,
    vsend, vrecv, prm,
    lsem, s1, s2, s3, s5, s6, s7, sv, sp, r1, r2, r3, r5, r6, r7, rv, rp, hello,
):
    def turn(i, d, n):
        return lax.rem(i + d, n)

    chan, slab = lax.axis_index("chan"), lax.axis_index("slab")
    mx, my = lax.div(chan, 4), lax.rem(chan, 4)
    mp, me = lax.div(my, 2), lax.rem(my, 2)
    mk, mh, z = lax.rem(slab, 2), lax.rem(lax.div(slab, 2), 2), lax.div(slab, 4)
    mz = z * 2 + mk
    mo = mx * 2 + me
    xs, ys = [turn(mx, d, 4) for d in range(4)], [turn(my, d, 4) for d in range(4)]
    ks, es = [mk, 1 - mk], [me, 1 - me]
    ring = [turn(mh * 4 + my, d, 8) for d in range(8)]
    x_rows = [lax.div(x, 2) * 16 + lax.rem(x, 2) * 4 for x in xs]
    FAR = (2, 3, 1, 0)

    chan_peers = [
        (xs[i] * 4 + ys[j], {"chan": xs[i] * 4 + ys[j]}) for i in FAR for j in FAR if i or j]
    y_peers = []
    for j in (4, 3, 5, 2, 6, 1, 7, 0):
        half, y = lax.div(ring[j], 4), lax.rem(ring[j], 4)
        side, there = half * 8 + lax.rem(y, 2), slab + 2 * (half - mh)
        for i in FAR:
            if i or j:
                y_peers.append((side + xs[i] * 2, x_rows[i] + half * 8 + y,
                                {"chan": xs[i] * 4 + y, "slab": there}))
    z_peers = []
    for d in (4, 3, 5, 2, 6, 1, 7, 0):
        for k in (1, 0):
            if d or k:
                far = turn(z, d, 8)
                z_peers.append((far * 2 + ks[k], {"slab": far * 4 + mh * 2 + ks[k]}))
    my_row, my_u = x_rows[0] + mh * 8 + my, mh * 8 + mo

    barrier = pltpu.get_barrier_semaphore()
    allies = [{"chan": xs[i] * 4 + mp * 2 + es[e]} for i in (2, 3, 1) for e in (1, 0)]
    ring_near = [{"chan": mx * 4 + lax.rem(ring[j], 4), "slab": slab + 2 * (lax.div(ring[j], 4) - mh)}
                 for j in (3, 5, 2, 6, 1, 7)]

    def z_at(d, k):
        return {"slab": turn(z, d, 8) * 4 + mh * 2 + ks[k]}

    z_near = [z_at(3, 0), z_at(5, 0), z_at(2, 0), z_at(6, 0), z_at(1, 1), z_at(7, 1), z_at(1, 0), z_at(7, 0), z_at(0, 1)]
    near = [peer[-1] for peer in chan_peers] + ring_near + z_near
    for device in near:
        pl.semaphore_signal(barrier, inc=1, device_id=device, device_id_type=MESH)

    loads = [
        pltpu.make_async_copy(src, dst, lsem.at[i])
        for i, (src, dst) in enumerate(
            [(taylor, tay_v), (vis, vis_v), (wt, wt_v), (t_a, va), (w_a, vwa),
             (t_b, vb), (t_d, vd), (w_d, vwd), (t_e, ve), (freq, freq_s), (robust, robust_s)]
        )
    ]
    for i in (9, 10, 0, 1, 2, 3, 4, 5, 6, 7, 8):
        loads[i].start()

    rows = lax.broadcasted_iota(jnp.int32, (8, 128), 0)
    loads[9].wait()
    loads[10].wait()
    prm[pl.ds(mo, 1)] = jnp.where(rows == 0, freq_s[0] - 1.0, robust_s[0])[None]
    loads[1].wait()
    loads[2].wait()
    for q in range(4):
        for p in range(3):
            src = wt_v[16 * q : 16 * q + 16] if p == 2 else vis_v[p, 16 * q : 16 * q + 16]
            wide = src.astype(F32)
            vsend[2 * q, p] = wide[:8]
            vsend[2 * q + 1, p] = wide[8:]
    loads[0].wait()

    pl.semaphore_wait(barrier, len(near))

    told = allies + [{"chan": mx * 4 + mp * 2 + es[1]}, z_at(0, 1), z_at(7, 0), z_at(7, 1)]
    for device in told:
        pl.semaphore_signal(hello, inc=1, device_id=device, device_id_type=MESH)

    def tile(ref, i, n=8):
        return ref.at[pl.ds(pl.multiple_of(i * n, n), n)]

    def spread(peers, src, dst, mine, kept, n, send, recv, which=0):
        for peer in peers:
            pltpu.make_async_remote_copy(
                tile(src, peer[which], n), tile(dst, mine, n), send, recv,
                device_id=peer[-1], device_id_type=MESH).start()
        pltpu.make_async_copy(tile(src, kept, n), tile(dst, mine, n), recv).start()

    def landed(buf, sem):
        pltpu.make_async_copy(buf, buf, sem).wait()

    def ally(d):
        x, e = xs[d // 2], es[d % 2]
        return x * 2 + e, {"chan": x * 4 + mp * 2 + e}

    def xp(d):
        return pltpu.make_async_remote_copy(
            prm.at[mo], prm.at[mo], sp, rp.at[d], device_id=ally(d)[1], device_id_type=MESH)

    def xv(which):
        for d, p in which:
            o, device = ally(d)
            pltpu.make_async_remote_copy(
                vsend.at[o, p], vrecv.at[d - 1, p], sv, rv.at[d],
                device_id=device, device_id_type=MESH).start()

    def arrived(d):
        xp(d).wait_recv()
        landed(vrecv.at[d - 1], rv.at[d])

    spread(chan_peers, tay_v, buf1, chan, chan, 8, s1, r1)

    for d in EARLY + LATE:
        xp(d).start()
    xv(SECOND)

    def put(dst, x):
        dst[0], dst[1] = split(x)

    for i in (3, 4, 5):
        loads[i].wait()
    put(ma, va[...])
    put(mb, vb[...])

    landed(buf1, r1)
    low = lax.broadcasted_iota(jnp.int32, (128, 128), 1) < 64
    pre = dot3(both(ma), split(buf1[...]), False)
    re, im = pre[:128], pre[128:]
    yre = re * vwa[0] - im * vwa[1]
    yim = re * vwa[1] + im * vwa[0]
    pre = dot3(both(mb), split(jnp.concatenate([yre, yim], axis=1)), True)
    re, im = pre[:128], pre[128:]
    snd2[pl.ds(0, 128, stride=2)] = jnp.where(low, re, swap(im))
    snd2[pl.ds(1, 128, stride=2)] = jnp.where(low, swap(re), im)

    pl.semaphore_wait(hello, len(told))

    spread(z_peers, snd2, buf2, mz, mz, 16, s2, r2)

    for i in (6, 7, 8):
        loads[i].wait()
    put(md, vd[...])
    put(me2, ve[...])
    put(mat, va[...].T)
    put(met, ve[...].T)
    put(mdt, jnp.concatenate([vd[:256].T, vd[256:].T], axis=0))
    vwdt[0] = vwd[0, :, :].T
    vwdt[1] = vwd[1, :, :].T

    landed(buf2, r2)
    for i in range(16):
        snd3[16 * i : 16 * i + 16] = buf2[pl.ds(i, 16, stride=16)]

    spread(y_peers, snd3, buf3, my_row, my_u, 16, s3, r3)
    xv(THIRD)
    landed(buf3, r3)

    x = jnp.concatenate([buf3[:256], buf3[256:]], axis=1)
    pre = dot3(both(md), split(x), False)
    sign = jnp.where(lax.broadcasted_iota(jnp.int32, (256, 128), 1) < 64, 1.0, -1.0)
    parts = []
    for t in range(2):
        lanes = slice(128 * t, 128 * t + 128)
        y = pre[:256, lanes] + sign * swap(pre[256:, lanes])
        parts.append(y * vwd[0] + swap(y) * vwd[1])
    fs[...] = dot3(both(me2), split(jnp.concatenate(parts, axis=0)), True)

    def point(first, group, m, _):
        lo, hi = pl.ds(pl.multiple_of(8 * m, 8), 8), pl.ds(pl.multiple_of(64 + 8 * m, 8), 8)
        lane = pl.ds(pl.multiple_of(256 * m, 256), 256)
        f0r, f1r = fs[lo, :256], fs[lo, 256:]
        f0i, f1i = fs[hi, :256], fs[hi, 256:]
        if first:
            sums = [jnp.zeros((8, 256), F32)] * 4
        else:
            sums = [ws[lo, :256], ws[hi, :256], ws[lo, 256:], ws[hi, 256:]]
        for d in group:
            who = turn(mx, 4 - d // 2, 4) * 2 + es[d % 2]
            pair = prm[pl.ds(who, 1)][0]
            off, damp = pair[0:1, 0:1], pair[1:2, 0:1]
            if d == 0:
                vr, vi, w = (vsend[pl.ds(mo, 1), p, :, lane][0] for p in range(3))
            else:
                vr, vi, w = (vrecv[d - 1, p, :, lane] for p in range(3))
            dr = vr - w * (f0r + off * f1r)
            di = vi - w * (f0i + off * f1i)
            k = 1.0 / (1.0 + damp * (dr * dr + di * di))
            wr, wi = k * dr, k * di
            sums = [sums[0] + wr, sums[1] + wi, sums[2] + off * wr, sums[3] + off * wi]
        ws[lo, :256], ws[hi, :256], ws[lo, 256:], ws[hi, 256:] = sums
        return 0

    for d in EARLY:
        arrived(d)
    lax.fori_loop(0, 8, functools.partial(point, True, (0,) + EARLY), 0, unroll=True)
    for d in LATE:
        arrived(d)
    lax.fori_loop(0, 8, functools.partial(point, False, LATE), 0, unroll=True)

    pre = dot3(both(met), split(ws[...]), False)
    parts = []
    for t in range(2):
        re, im = pre[:64, 256 * t : 256 * t + 256], pre[64:, 256 * t : 256 * t + 256]
        parts += [re * vwdt[0, :64] - im * vwdt[1, :64], im * vwdt[0, :64] + re * vwdt[1, :64]]
    back = dot3(both(mdt), split(jnp.concatenate(parts, axis=0)), True)
    for t in range(2):
        lanes = slice(128 * t, 128 * t + 128)
        snd5[256 * t : 256 * t + 256] = back[:256, lanes] - sign * swap(back[256:, lanes])

    spread(y_peers, snd5, buf5, mp * 16 + my_u, my_row, 16, s5, r5, 1)
    landed(buf5, r5)
    for i in range(16):
        b = 16 * i
        snd6[pl.ds(i, 16, stride=16)] = buf5[b : b + 16] + buf5[256 + b : 272 + b]

    spread(z_peers, snd6, buf6, mz, mz, 16, s6, r6)
    landed(buf1.at[: 8 * (NC - 1)], s1)
    landed(buf2.at[: 16 * (NZ - 1)], s2)
    landed(buf3.at[: 16 * (NY - 1)], s3)
    landed(buf5.at[: 16 * (NY - 1)], s5)
    landed(prm.at[:7], sp)
    landed(vrecv, sv)
    landed(buf6, r6)
    p0, p1 = buf6[pl.ds(0, 128, stride=2)], buf6[pl.ds(1, 128, stride=2)]
    re, im = jnp.where(low, p0, swap(p1)), jnp.where(low, swap(p0), p1)
    z = dot3(split(jnp.concatenate([re.T, im.T], axis=1)), both(mb), False)
    re, im = z[:, :128], z[:, 128:]
    z = jnp.concatenate([re * vwa[0] + im * vwa[1], im * vwa[0] - re * vwa[1]], axis=0)
    snd7[...] = dot3(both(mat), split(z), False)

    spread(chan_peers, snd7, buf7, chan, chan, 8, s7, r7)
    landed(buf7, r7)
    landed(buf6.at[: 16 * (NZ - 1)], s6)
    landed(buf7.at[: 8 * (NC - 1)], s7)
    out[...] = buf7[...]


def local(taylor_models, gridded_vis, uv_weight, freq_ratio, robust_scale):
    tabs = [jnp.asarray(x) for x in tables()]
    any_space = pl.BlockSpec(memory_space=pltpu.HBM)
    v = pltpu.VMEM
    dma = pltpu.SemaphoreType.DMA
    scratch = (
        [pltpu.SMEM((1,), F32), pltpu.SMEM((1,), F32), v((128, 128), F32), v((2, 64, PIX), BF16), v((64, PIX), BF16)]
        + [v(x.shape, F32) for x in tabs]
        + [v((2, *s), BF16) for s in
           ((256, 128), (128, 256), (256, 256), (512, 256), (512, 256), (128, 128), (128, 128))]
        + [v((2, 128, 256), F32)]
        + [v((n, m), F32) for n, m in
           ((128, 128), (256, 128), (256, 128), (256, 128), (512, 128), (128, 512), (128, 512),
            (512, 128), (512, 128), (256, 128), (256, 128), (128, 128), (128, 128))]
        + [v((8, 3, 8, PIX), F32), v((7, 3, 8, PIX), F32), v((8, 8, 128), F32)]
        + [dma((11,))] + [dma] * 8 + [dma] * 6 + [dma((8,)), dma((8,))] + [pltpu.SemaphoreType.REGULAR]
    )
    out = pl.pallas_call(
        kernel,
        out_shape=pltpu.VMEM((128, 128), F32),
        in_specs=[any_space] * 11,
        out_specs=pl.BlockSpec(memory_space=pltpu.VMEM),
        scratch_shapes=scratch,
        compiler_params=pltpu.CompilerParams(
            collective_id=0, has_side_effects=True, vmem_limit_bytes=66_000_000),
    )(freq_ratio, robust_scale, taylor_models.reshape(128, 128), gridded_vis[0], uv_weight[0], *tabs)
    return out.reshape(2, 64, 128)


def solution(mesh):
    placed = (
        P(None, "slab", "chan"),
        P("chan", None, "slab", None),
        P("chan", "slab", None),
        P("chan"),
        P("chan"),
    )
    return jax.shard_map(
        local, mesh=mesh, in_specs=placed, out_specs=P(None, "slab", "chan"), check_vma=False
    )
```

```python
import functools

import jax
import jax.numpy as jnp
import numpy as np
from jax import lax
from jax.experimental import pallas as pl
from jax.experimental.pallas import tpu as pltpu
from jax.sharding import PartitionSpec as P

PIX = 2048
F32, BF16 = jnp.float32, jnp.bfloat16
MESH = pl.DeviceIdType.MESH
NC, NZ, NY = 16, 16, 32


THIRD = ((7, 1), (7, 2))
SECOND = tuple((d, p) for d in (1, 5, 4, 2, 6, 3, 7) for p in range(3) if (d, p) not in THIRD)
EARLY, LATE = (1, 5, 4, 2, 6, 3), (7,)


def rep(angle):
    c, s = np.cos(angle), np.sin(angle)
    return np.array([[c, s], [-s, c]])


def tables():
    tau = 2 * np.pi
    j, c = np.arange(16), np.arange(16)
    ang = tau * np.outer(j, c) / 16
    first = np.stack([np.cos(ang), -np.sin(ang)])
    t_a = np.einsum("ijc,rq->ijrcq", first, np.eye(8)).reshape(256, 128)
    ang = np.repeat(tau * np.outer(j, np.arange(128)) / PIX, 8, axis=0)
    w_a = np.stack([np.cos(ang), -np.sin(ang)])
    z, k, h, q = np.meshgrid(*map(np.arange, (8, 2, 2, 4)), indexing="ij")
    step = (((z * 2 + h) * 2 + k) * 4 + q).reshape(128)
    t_b = np.einsum("oika->okia", rep(tau * np.outer(step, np.arange(128)) / 128)).reshape(256, 256)
    h, g, z, k = np.meshgrid(*map(np.arange, (2, 8, 8, 2)), indexing="ij")
    y1 = (8 * ((z * 2 + h) * 2 + k) + g).reshape(256)
    ang = tau * (np.outer(np.arange(256), y1) % 256) / 256
    t_d = np.concatenate([np.cos(ang), np.sin(ang)])
    ang = np.tile(tau * np.outer(np.arange(256), np.arange(8)) / PIX, (1, 8))
    w_d = np.stack([np.tile(np.cos(ang), (1, 2)), np.concatenate([np.sin(ang), -np.sin(ang)], axis=1)]) / PIX
    e = rep(tau * np.outer(np.arange(8), np.arange(8)) / 8)
    t_e = np.einsum("oimr,jq->omjiqr", e, np.eye(8)).reshape(128, 128)
    return [x.astype(np.float32) for x in (t_a, w_a, t_b, t_d, w_d, t_e)]


def split(x):
    hi = x.astype(BF16)
    return hi, (x - hi.astype(F32)).astype(BF16)


def dot3(a, b, nt):
    dims = (((1,), (1 if nt else 0,)), ((), ()))

    def one(p, q):
        return lax.dot_general(p, q, dims, preferred_element_type=F32)

    return one(a[0], b[0]) + one(a[0], b[1]) + one(a[1], b[0])


def both(ref):
    return ref[0], ref[1]


def swap(x):
    return pltpu.roll(x, 64, axis=1)


def kernel(
    freq, robust, taylor, vis, wt, t_a, w_a, t_b, t_d, w_d, t_e, out,
    freq_s, robust_s, tay_v, vis_v, wt_v, va, vwa, vb, vd, vwd, ve,
    ma, mat, mb, md, mdt, me2, met, vwdt,
    buf1, snd2, buf2, snd3, buf3, fs, ws, snd5, buf5, snd6, buf6, snd7, buf7,
    vsend, vrecv, prm,
    lsem, s1, s2, s3, s5, s6, s7, sv, sp, r1, r2, r3, r5, r6, r7, rv, rp, hello,
):
    def turn(i, d, n):
        return lax.rem(i + d, n)

    chan, slab = lax.axis_index("chan"), lax.axis_index("slab")
    mx, my = lax.div(chan, 4), lax.rem(chan, 4)
    mp, me = lax.div(my, 2), lax.rem(my, 2)
    mk, mh, z = lax.rem(slab, 2), lax.rem(lax.div(slab, 2), 2), lax.div(slab, 4)
    mz = z * 2 + mk
    mo = mx * 2 + me
    xs, ys = [turn(mx, d, 4) for d in range(4)], [turn(my, d, 4) for d in range(4)]
    ks, es = [mk, 1 - mk], [me, 1 - me]
    ring = [turn(mh * 4 + my, d, 8) for d in range(8)]
    x_rows = [lax.div(x, 2) * 16 + lax.rem(x, 2) * 4 for x in xs]
    FAR = (2, 3, 1, 0)

    chan_peers = [
        (xs[i] * 4 + ys[j], {"chan": xs[i] * 4 + ys[j]}) for i in FAR for j in FAR if i or j]
    y_peers = []
    for j in (4, 3, 5, 2, 6, 1, 7, 0):
        half, y = lax.div(ring[j], 4), lax.rem(ring[j], 4)
        side, there = half * 8 + lax.rem(y, 2), slab + 2 * (half - mh)
        for i in FAR:
            if i or j:
                y_peers.append((side + xs[i] * 2, x_rows[i] + half * 8 + y,
                                {"chan": xs[i] * 4 + y, "slab": there}))
    z_peers = []
    for d in (4, 3, 5, 2, 6, 1, 7, 0):
        for k in (1, 0):
            if d or k:
                far = turn(z, d, 8)
                z_peers.append((far * 2 + ks[k], {"slab": far * 4 + mh * 2 + ks[k]}))
    my_row, my_u = x_rows[0] + mh * 8 + my, mh * 8 + mo

    barrier = pltpu.get_barrier_semaphore()
    allies = [{"chan": xs[i] * 4 + mp * 2 + es[e]} for i in (2, 3, 1) for e in (1, 0)]
    ring_near = [{"chan": mx * 4 + lax.rem(ring[j], 4), "slab": slab + 2 * (lax.div(ring[j], 4) - mh)}
                 for j in (3, 5, 2, 6, 1, 7)]

    def z_at(d, k):
        return {"slab": turn(z, d, 8) * 4 + mh * 2 + ks[k]}

    z_near = [z_at(3, 0), z_at(5, 0), z_at(2, 0), z_at(6, 0), z_at(1, 1), z_at(7, 1), z_at(1, 0), z_at(7, 0), z_at(0, 1)]
    near = [peer[-1] for peer in chan_peers] + ring_near + z_near
    for device in near:
        pl.semaphore_signal(barrier, inc=1, device_id=device, device_id_type=MESH)

    loads = [
        pltpu.make_async_copy(src, dst, lsem.at[i])
        for i, (src, dst) in enumerate(
            [(taylor, tay_v), (vis, vis_v), (wt, wt_v), (t_a, va), (w_a, vwa),
             (t_b, vb), (t_d, vd), (w_d, vwd), (t_e, ve), (freq, freq_s), (robust, robust_s)]
        )
    ]
    for i in (9, 10, 0, 1, 2, 3, 4, 5, 6, 7, 8):
        loads[i].start()

    rows = lax.broadcasted_iota(jnp.int32, (8, 128), 0)
    loads[9].wait()
    loads[10].wait()
    prm[pl.ds(mo, 1)] = jnp.where(rows == 0, freq_s[0] - 1.0, robust_s[0])[None]
    loads[1].wait()
    loads[2].wait()
    for q in range(4):
        for p in range(3):
            src = wt_v[16 * q : 16 * q + 16] if p == 2 else vis_v[p, 16 * q : 16 * q + 16]
            wide = src.astype(F32)
            vsend[2 * q, p] = wide[:8]
            vsend[2 * q + 1, p] = wide[8:]
    loads[0].wait()

    pl.semaphore_wait(barrier, len(near))

    told = allies + [{"chan": mx * 4 + mp * 2 + es[1]}, z_at(0, 1), z_at(7, 0), z_at(7, 1)]
    for device in told:
        pl.semaphore_signal(hello, inc=1, device_id=device, device_id_type=MESH)

    def tile(ref, i, n=8):
        return ref.at[pl.ds(pl.multiple_of(i * n, n), n)]

    def spread(peers, src, dst, mine, kept, n, send, recv, which=0):
        for peer in peers:
            pltpu.make_async_remote_copy(
                tile(src, peer[which], n), tile(dst, mine, n), send, recv,
                device_id=peer[-1], device_id_type=MESH).start()
        pltpu.make_async_copy(tile(src, kept, n), tile(dst, mine, n), recv).start()

    def landed(buf, sem):
        pltpu.make_async_copy(buf, buf, sem).wait()

    def ally(d):
        x, e = xs[d // 2], es[d % 2]
        return x * 2 + e, {"chan": x * 4 + mp * 2 + e}

    def xp(d):
        return pltpu.make_async_remote_copy(
            prm.at[mo], prm.at[mo], sp, rp.at[d], device_id=ally(d)[1], device_id_type=MESH)

    def xv(which):
        for d, p in which:
            o, device = ally(d)
            pltpu.make_async_remote_copy(
                vsend.at[o, p], vrecv.at[d - 1, p], sv, rv.at[d],
                device_id=device, device_id_type=MESH).start()

    def arrived(d):
        xp(d).wait_recv()
        landed(vrecv.at[d - 1], rv.at[d])

    spread(chan_peers, tay_v, buf1, chan, chan, 8, s1, r1)

    for d in EARLY + LATE:
        xp(d).start()
    xv(SECOND)

    def put(dst, x):
        dst[0], dst[1] = split(x)

    for i in (3, 4, 5):
        loads[i].wait()
    put(ma, va[...])
    put(mb, vb[...])

    landed(buf1, r1)
    low = lax.broadcasted_iota(jnp.int32, (128, 128), 1) < 64
    pre = dot3(both(ma), split(buf1[...]), False)
    re, im = pre[:128], pre[128:]
    yre = re * vwa[0] - im * vwa[1]
    yim = re * vwa[1] + im * vwa[0]
    pre = dot3(both(mb), split(jnp.concatenate([yre, yim], axis=1)), True)
    re, im = pre[:128], pre[128:]
    snd2[pl.ds(0, 128, stride=2)] = jnp.where(low, re, swap(im))
    snd2[pl.ds(1, 128, stride=2)] = jnp.where(low, swap(re), im)

    pl.semaphore_wait(hello, len(told))

    spread(z_peers, snd2, buf2, mz, mz, 16, s2, r2)

    for i in (6, 7, 8):
        loads[i].wait()
    put(md, vd[...])
    put(me2, ve[...])
    put(mat, va[...].T)
    put(met, ve[...].T)
    turned = (vd[:256].T, vd[256:].T)
    for a in range(2):
        put(mdt.at[a], jnp.concatenate(
            [x[16 * i + 8 * a : 16 * i + 8 * a + 8] for x in turned for i in range(16)], axis=0))
    vwdt[0] = vwd[0, :, :].T
    vwdt[1] = vwd[1, :, :].T

    landed(buf2, r2)
    for i in range(16):
        snd3[16 * i : 16 * i + 16] = buf2[pl.ds(i, 16, stride=16)]

    spread(y_peers, snd3, buf3, my_row, my_u, 16, s3, r3)
    xv(THIRD)
    landed(buf3, r3)

    x = jnp.concatenate([buf3[:256], buf3[256:]], axis=1)
    pre = dot3(both(md), split(x), False)
    sign = jnp.where(lax.broadcasted_iota(jnp.int32, (256, 128), 1) < 64, 1.0, -1.0)
    parts = []
    for t in range(2):
        lanes = slice(128 * t, 128 * t + 128)
        y = pre[:256, lanes] + sign * swap(pre[256:, lanes])
        parts.append(y * vwd[0] + swap(y) * vwd[1])
    fs[...] = dot3(both(me2), split(jnp.concatenate(parts, axis=0)), True)

    def point(first, group, m, _):
        lo, hi = pl.ds(pl.multiple_of(8 * m, 8), 8), pl.ds(pl.multiple_of(64 + 8 * m, 8), 8)
        lane = pl.ds(pl.multiple_of(256 * m, 256), 256)
        f0r, f1r = fs[lo, :256], fs[lo, 256:]
        f0i, f1i = fs[hi, :256], fs[hi, 256:]
        if first:
            sums = [jnp.zeros((8, 256), F32)] * 4
        else:
            sums = [ws[lo, :256], ws[hi, :256], ws[lo, 256:], ws[hi, 256:]]
        for d in group:
            who = turn(mx, 4 - d // 2, 4) * 2 + es[d % 2]
            pair = prm[pl.ds(who, 1)][0]
            off, damp = pair[0:1, 0:1], pair[1:2, 0:1]
            if d == 0:
                vr, vi, w = (vsend[pl.ds(mo, 1), p, :, lane][0] for p in range(3))
            else:
                vr, vi, w = (vrecv[d - 1, p, :, lane] for p in range(3))
            dr = vr - w * (f0r + off * f1r)
            di = vi - w * (f0i + off * f1i)
            k = 1.0 / (1.0 + damp * (dr * dr + di * di))
            wr, wi = k * dr, k * di
            sums = [sums[0] + wr, sums[1] + wi, sums[2] + off * wr, sums[3] + off * wi]
        ws[lo, :256], ws[hi, :256], ws[lo, 256:], ws[hi, 256:] = sums
        return 0

    for d in EARLY:
        arrived(d)
    lax.fori_loop(0, 8, functools.partial(point, True, (0,) + EARLY), 0, unroll=True)
    for d in LATE:
        arrived(d)
    lax.fori_loop(0, 8, functools.partial(point, False, LATE), 0, unroll=True)

    pre = dot3(both(met), split(ws[...]), False)
    parts = []
    for t in range(2):
        re, im = pre[:64, 256 * t : 256 * t + 256], pre[64:, 256 * t : 256 * t + 256]
        parts += [re * vwdt[0, :64] - im * vwdt[1, :64], im * vwdt[0, :64] + re * vwdt[1, :64]]
    y = split(jnp.concatenate(parts, axis=0))
    far_half = 1 - lax.div(z, 4)
    halves = (far_half, 1 - far_half)
    sign = sign[:128]

    mine = mp * 16 + my_u
    for o, a in enumerate(halves):
        back = dot3((mdt[a, 0], mdt[a, 1]), y, True)
        for t in range(2):
            lanes = slice(128 * t, 128 * t + 128)
            snd5[o, 128 * t : 128 * t + 128] = back[:128, lanes] - sign * swap(back[128:, lanes])
        spread(y_peers, snd5.at[o], buf5.at[o], mine, my_row, 8, s5.at[o], r5.at[o], 1)

    for o, a in enumerate(halves):
        landed(buf5.at[o], r5.at[o])
        for i in range(16):
            b = 8 * i
            snd6[o, pl.ds(i, 8, stride=16)] = buf5[o, b : b + 8] + buf5[o, 128 + b : 136 + b]
        own = lax.rem(mz, 8)
        for d in (4, 3, 5, 2, 6, 1, 7, 0):
            n = turn(own, d, 8)
            if d or o == 0:
                pltpu.make_async_remote_copy(
                    tile(snd6.at[o], n, 16), tile(buf6, mz, 16), s6, r6,
                    device_id={"slab": (a * 4 + lax.div(n, 2)) * 4 + mh * 2 + lax.rem(n, 2)},
                    device_id_type=MESH).start()
            else:
                pltpu.make_async_copy(tile(snd6.at[o], n, 16), tile(buf6, mz, 16), r6).start()
    landed(buf1.at[: 8 * (NC - 1)], s1)
    landed(buf2.at[: 16 * (NZ - 1)], s2)
    landed(buf3.at[: 16 * (NY - 1)], s3)
    for o in range(2):
        landed(buf5.at[o, : 8 * (NY - 1)], s5.at[o])
    landed(prm.at[:7], sp)
    landed(vrecv, sv)
    landed(buf6, r6)
    p0, p1 = buf6[pl.ds(0, 128, stride=2)], buf6[pl.ds(1, 128, stride=2)]
    re, im = jnp.where(low, p0, swap(p1)), jnp.where(low, swap(p0), p1)
    z = dot3(split(jnp.concatenate([re.T, im.T], axis=1)), both(mb), False)
    re, im = z[:, :128], z[:, 128:]
    z = jnp.concatenate([re * vwa[0] + im * vwa[1], im * vwa[0] - re * vwa[1]], axis=0)
    snd7[...] = dot3(both(mat), split(z), False)

    spread(chan_peers, snd7, buf7, chan, chan, 8, s7, r7)
    landed(buf7, r7)
    landed(buf6.at[: 16 * (NZ - 1)], s6)
    landed(buf7.at[: 8 * (NC - 1)], s7)
    out[...] = buf7[...]


def local(taylor_models, gridded_vis, uv_weight, freq_ratio, robust_scale):
    tabs = [jnp.asarray(x) for x in tables()]
    any_space = pl.BlockSpec(memory_space=pltpu.HBM)
    v = pltpu.VMEM
    dma = pltpu.SemaphoreType.DMA
    scratch = (
        [pltpu.SMEM((1,), F32), pltpu.SMEM((1,), F32), v((128, 128), F32), v((2, 64, PIX), BF16), v((64, PIX), BF16)]
        + [v(x.shape, F32) for x in tabs]
        + [v((2, *s), BF16) for s in
           ((256, 128), (128, 256), (256, 256), (512, 256), (2, 256, 256), (128, 128), (128, 128))]
        + [v((2, 128, 256), F32)]
        + [v(s, F32) for s in
           ((128, 128), (256, 128), (256, 128), (256, 128), (512, 128), (128, 512), (128, 512),
            (2, 256, 128), (2, 256, 128), (2, 128, 128), (256, 128), (128, 128), (128, 128))]
        + [v((8, 3, 8, PIX), F32), v((7, 3, 8, PIX), F32), v((8, 8, 128), F32)]
        + [dma((11,)), dma, dma, dma, dma((2,)), dma, dma, dma, dma, dma, dma, dma, dma((2,)), dma, dma, dma((8,)), dma((8,))] + [pltpu.SemaphoreType.REGULAR]
    )
    out = pl.pallas_call(
        kernel,
        out_shape=pltpu.VMEM((128, 128), F32),
        in_specs=[any_space] * 11,
        out_specs=pl.BlockSpec(memory_space=pltpu.VMEM),
        scratch_shapes=scratch,
        compiler_params=pltpu.CompilerParams(
            collective_id=0, has_side_effects=True, vmem_limit_bytes=66_000_000),
    )(freq_ratio, robust_scale, taylor_models.reshape(128, 128), gridded_vis[0], uv_weight[0], *tabs)
    return out.reshape(2, 64, 128)


def solution(mesh):
    placed = (
        P(None, "slab", "chan"),
        P("chan", None, "slab", None),
        P("chan", "slab", None),
        P("chan"),
        P("chan"),
    )
    return jax.shard_map(
        local, mesh=mesh, in_specs=placed, out_specs=P(None, "slab", "chan"), check_vma=False
    )
```

```python
import functools

import jax
import jax.numpy as jnp
import numpy as np
from jax import lax
from jax.experimental import pallas as pl
from jax.experimental.pallas import tpu as pltpu
from jax.sharding import PartitionSpec as P

PIX = 2048
F32, BF16 = jnp.float32, jnp.bfloat16
MESH = pl.DeviceIdType.MESH
NC, NZ, NY = 16, 16, 32


THIRD = ((7, 2),)
SECOND = tuple((d, p) for d in (1, 5, 4, 2, 6, 3, 7) for p in range(3) if (d, p) not in THIRD)
EARLY, LATE = (1, 5, 4, 2, 6, 3), (7,)


def rep(angle):
    c, s = np.cos(angle), np.sin(angle)
    return np.array([[c, s], [-s, c]])


def tables():
    tau = 2 * np.pi
    j, c = np.arange(16), np.arange(16)
    ang = (tau * np.outer(j, c) / 16).reshape(2, 8, 16)
    first = np.stack([np.cos(ang), -np.sin(ang)])
    t_a = np.einsum("iejc,rq->ierjcq", first, np.eye(8)).reshape(256, 128)
    ang = np.repeat(tau * np.outer(j, np.arange(128)) / PIX, 8, axis=0)
    w_a = np.stack([np.cos(ang), -np.sin(ang)])
    w_b = w_a.reshape(2, 2, 8, 8, 128).swapaxes(2, 3).reshape(2, 128, 128)
    z, k, h, q = np.meshgrid(*map(np.arange, (8, 2, 2, 4)), indexing="ij")
    step = (((z * 2 + h) * 2 + k) * 4 + q).reshape(128)
    t_b = np.einsum("oika->okia", rep(tau * np.outer(step, np.arange(128)) / 128)).reshape(256, 256)
    h, g, z, k = np.meshgrid(*map(np.arange, (2, 8, 8, 2)), indexing="ij")
    y1 = (8 * ((z * 2 + h) * 2 + k) + g).reshape(256)
    ang = tau * (np.outer(np.arange(256), y1) % 256) / 256
    t_d = np.concatenate([np.cos(ang), np.sin(ang)])
    ang = np.tile(tau * np.outer(np.arange(256), np.arange(8)) / PIX, (1, 8))
    w_d = np.stack([np.tile(np.cos(ang), (1, 2)), np.concatenate([np.sin(ang), -np.sin(ang)], axis=1)]) / PIX
    e = rep(tau * np.outer(np.arange(8), np.arange(8)) / 8)
    t_e = np.einsum("oimr,jq->omjiqr", e, np.eye(8)).reshape(128, 128)
    return [x.astype(np.float32) for x in (t_a, w_a, t_b, t_d, w_d, t_e, w_b)]


def combine(a, b, sign):
    if b is None:
        return a
    if a is None:
        return b if sign > 0 else -b
    return a + b if sign > 0 else a - b


def twist(x, k, n, sign):
    re, im = x
    if k == 0:
        return x
    if 4 * k == n:
        return (None if im is None else -sign * im, sign * re)
    c, s = float(np.cos(2 * np.pi * k / n)), float(sign * np.sin(2 * np.pi * k / n))
    if im is None:
        return c * re, s * re
    return c * re - s * im, c * im + s * re


def transform(xs, sign):
    n = len(xs)
    if n == 1:
        return xs
    even, odd = transform(xs[::2], sign), transform(xs[1::2], sign)
    odd = [twist(x, k, n, sign) for k, x in enumerate(odd)]
    return [tuple(combine(p, q, side) for p, q in zip(a, b)) for side in (1, -1) for a, b in zip(even, odd)]


def split(x):
    hi = x.astype(BF16)
    return hi, (x - hi.astype(F32)).astype(BF16)


def dot3(a, b, nt):
    dims = (((1,), (1 if nt else 0,)), ((), ()))

    def one(p, q):
        return lax.dot_general(p, q, dims, preferred_element_type=F32)

    return one(a[0], b[0]) + one(a[0], b[1]) + one(a[1], b[0])


def both(ref):
    return ref[0], ref[1]


def swap(x):
    return pltpu.roll(x, 64, axis=1)


def kernel(
    freq, robust, taylor, vis, wt, t_a, w_a, t_b, t_d, w_d, t_e, w_b, out,
    freq_s, robust_s, tay_v, vis_v, wt_v, va, vwa, vb, vd, vwd, ve, vwb,
    mat, mb, md, mdt, me2, vwdt,
    buf1, snd2, buf2, snd3, buf3, fs, ws, snd5, buf5, snd6, buf6, snd7, buf7,
    vsend, vrecv, prm,
    lsem, s1, s2, s3, s5, s6, s7, sv, sp, r1, r2, r3, r5, r6, r7, rv, rp, hello,
):
    def turn(i, d, n):
        return lax.rem(i + d, n)

    chan, slab = lax.axis_index("chan"), lax.axis_index("slab")
    mx, my = lax.div(chan, 4), lax.rem(chan, 4)
    mp, me = lax.div(my, 2), lax.rem(my, 2)
    mk, mh, z = lax.rem(slab, 2), lax.rem(lax.div(slab, 2), 2), lax.div(slab, 4)
    mz = z * 2 + mk
    mo = mx * 2 + me
    xs, ys = [turn(mx, d, 4) for d in range(4)], [turn(my, d, 4) for d in range(4)]
    ks, es = [mk, 1 - mk], [me, 1 - me]
    ring = [turn(mh * 4 + my, d, 8) for d in range(8)]
    x_rows = [lax.div(x, 2) * 16 + lax.rem(x, 2) * 4 for x in xs]
    FAR = (2, 3, 1, 0)

    chan_peers = [
        (xs[i] * 4 + ys[j], {"chan": xs[i] * 4 + ys[j]}) for i in FAR for j in FAR if i or j]
    y_peers = []
    for j in (4, 3, 5, 2, 6, 1, 7, 0):
        half, y = lax.div(ring[j], 4), lax.rem(ring[j], 4)
        side, there = half * 8 + lax.rem(y, 2), slab + 2 * (half - mh)
        for i in FAR:
            if i or j:
                y_peers.append((side + xs[i] * 2, x_rows[i] + half * 8 + y,
                                {"chan": xs[i] * 4 + y, "slab": there}))
    z_peers = []
    for d in (4, 3, 5, 2, 6, 1, 7, 0):
        for k in (1, 0):
            if d or k:
                far = turn(z, d, 8)
                z_peers.append((far * 2 + ks[k], {"slab": far * 4 + mh * 2 + ks[k]}))
    my_row, my_u = x_rows[0] + mh * 8 + my, mh * 8 + mo

    barrier = pltpu.get_barrier_semaphore()
    allies = [{"chan": xs[i] * 4 + mp * 2 + es[e]} for i in (2, 3, 1) for e in (1, 0)]
    ring_near = [{"chan": mx * 4 + lax.rem(ring[j], 4), "slab": slab + 2 * (lax.div(ring[j], 4) - mh)}
                 for j in (3, 5, 2, 6, 1, 7)]

    def z_at(d, k):
        return {"slab": turn(z, d, 8) * 4 + mh * 2 + ks[k]}

    z_near = [z_at(3, 0), z_at(5, 0), z_at(2, 0), z_at(6, 0), z_at(1, 1), z_at(7, 1), z_at(1, 0), z_at(7, 0), z_at(0, 1)]
    near = [peer[-1] for peer in chan_peers] + ring_near + z_near
    for device in near:
        pl.semaphore_signal(barrier, inc=1, device_id=device, device_id_type=MESH)

    loads = [
        pltpu.make_async_copy(src, dst, lsem.at[i])
        for i, (src, dst) in enumerate(
            [(taylor, tay_v), (vis, vis_v), (wt, wt_v), (t_a, va), (w_a, vwa),
             (t_b, vb), (t_d, vd), (w_d, vwd), (t_e, ve), (freq, freq_s), (robust, robust_s), (w_b, vwb)]
        )
    ]
    for i in (9, 10, 0, 1, 2, 4, 5, 6, 7, 8, 3, 11):
        loads[i].start()

    rows = lax.broadcasted_iota(jnp.int32, (8, 128), 0)
    loads[9].wait()
    loads[10].wait()
    prm[pl.ds(mo, 1)] = jnp.where(rows == 0, freq_s[0] - 1.0, robust_s[0])[None]
    loads[1].wait()
    loads[2].wait()
    for q in range(4):
        for p in range(3):
            src = wt_v[16 * q : 16 * q + 16] if p == 2 else vis_v[p, 16 * q : 16 * q + 16]
            wide = src.astype(F32)
            vsend[2 * q, p] = wide[:8]
            vsend[2 * q + 1, p] = wide[8:]
    loads[0].wait()

    pl.semaphore_wait(barrier, len(near))

    told = allies + [{"chan": mx * 4 + mp * 2 + es[1]}, z_at(0, 1), z_at(7, 0), z_at(7, 1)]
    for device in told:
        pl.semaphore_signal(hello, inc=1, device_id=device, device_id_type=MESH)

    def tile(ref, i, n=8):
        return ref.at[pl.ds(pl.multiple_of(i * n, n), n)]

    def spread(peers, src, dst, mine, kept, n, send, recv, which=0):
        for peer in peers:
            pltpu.make_async_remote_copy(
                tile(src, peer[which], n), tile(dst, mine, n), send, recv,
                device_id=peer[-1], device_id_type=MESH).start()
        pltpu.make_async_copy(tile(src, kept, n), tile(dst, mine, n), recv).start()

    def landed(buf, sem):
        pltpu.make_async_copy(buf, buf, sem).wait()

    def ally(d):
        x, e = xs[d // 2], es[d % 2]
        return x * 2 + e, {"chan": x * 4 + mp * 2 + e}

    def xp(d):
        return pltpu.make_async_remote_copy(
            prm.at[mo], prm.at[mo], sp, rp.at[d], device_id=ally(d)[1], device_id_type=MESH)

    def xv(which):
        for d, p in which:
            o, device = ally(d)
            pltpu.make_async_remote_copy(
                vsend.at[o, p], vrecv.at[d - 1, p], sv, rv.at[d],
                device_id=device, device_id_type=MESH).start()

    def arrived(d):
        xp(d).wait_recv()
        landed(vrecv.at[d - 1], rv.at[d])

    spread(chan_peers, tay_v, buf1, chan, chan, 8, s1, r1)

    for d in EARLY + LATE:
        xp(d).start()
    xv(SECOND)

    def put(dst, x):
        dst[0], dst[1] = split(x)

    for i in (4, 5):
        loads[i].wait()
    put(mb, vb[...])

    landed(buf1, r1)
    low = lax.broadcasted_iota(jnp.int32, (128, 128), 1) < 64
    rows_in = [(buf1[8 * i : 8 * i + 8], None) for i in range(16)]
    rows_out = transform(rows_in, -1.0)
    re = jnp.concatenate([x[0] for x in rows_out], axis=0)
    im = jnp.concatenate([jnp.zeros((8, 128), F32) if x[1] is None else x[1] for x in rows_out], axis=0)
    yre = re * vwa[0] - im * vwa[1]
    yim = re * vwa[1] + im * vwa[0]
    pre = dot3(both(mb), split(jnp.concatenate([yre, yim], axis=1)), True)
    re, im = pre[:128], pre[128:]
    snd2[pl.ds(0, 128, stride=2)] = jnp.where(low, re, swap(im))
    snd2[pl.ds(1, 128, stride=2)] = jnp.where(low, swap(re), im)

    pl.semaphore_wait(hello, len(told))

    spread(z_peers, snd2, buf2, mz, mz, 16, s2, r2)

    for i in (6, 7, 8, 3, 11):
        loads[i].wait()
    put(md, vd[...])
    put(me2, ve[...])
    put(mat, va[...].T)
    turned = (vd[:256].T, vd[256:].T)
    for a in range(2):
        put(mdt.at[a], jnp.concatenate(
            [x[16 * i + 8 * a : 16 * i + 8 * a + 8] for x in turned for i in range(16)], axis=0))
    vwdt[0] = vwd[0, :, :].T
    vwdt[1] = vwd[1, :, :].T

    landed(buf2, r2)
    for i in range(16):
        snd3[16 * i : 16 * i + 16] = buf2[pl.ds(i, 16, stride=16)]

    spread(y_peers, snd3, buf3, my_row, my_u, 16, s3, r3)
    xv(THIRD)
    landed(buf3, r3)

    x = jnp.concatenate([buf3[:256], buf3[256:]], axis=1)
    pre = dot3(both(md), split(x), False)
    sign = jnp.where(lax.broadcasted_iota(jnp.int32, (256, 128), 1) < 64, 1.0, -1.0)
    parts = []
    for t in range(2):
        lanes = slice(128 * t, 128 * t + 128)
        y = pre[:256, lanes] + sign * swap(pre[256:, lanes])
        parts.append(y * vwd[0] + swap(y) * vwd[1])
    fs[...] = dot3(both(me2), split(jnp.concatenate(parts, axis=0)), True)

    def point(first, group, m, _):
        lo, hi = pl.ds(pl.multiple_of(8 * m, 8), 8), pl.ds(pl.multiple_of(64 + 8 * m, 8), 8)
        lane = pl.ds(pl.multiple_of(256 * m, 256), 256)
        f0r, f1r = fs[lo, :256], fs[lo, 256:]
        f0i, f1i = fs[hi, :256], fs[hi, 256:]
        if first:
            sums = [jnp.zeros((8, 256), F32)] * 4
        else:
            sums = [ws[lo, :256], ws[hi, :256], ws[lo, 256:], ws[hi, 256:]]
        for d in group:
            who = turn(mx, 4 - d // 2, 4) * 2 + es[d % 2]
            pair = prm[pl.ds(who, 1)][0]
            off, damp = pair[0:1, 0:1], pair[1:2, 0:1]
            if d == 0:
                vr, vi, w = (vsend[pl.ds(mo, 1), p, :, lane][0] for p in range(3))
            else:
                vr, vi, w = (vrecv[d - 1, p, :, lane] for p in range(3))
            dr = vr - w * (f0r + off * f1r)
            di = vi - w * (f0i + off * f1i)
            k = 1.0 / (1.0 + damp * (dr * dr + di * di))
            wr, wi = k * dr, k * di
            sums = [sums[0] + wr, sums[1] + wi, sums[2] + off * wr, sums[3] + off * wi]
        ws[lo, :256], ws[hi, :256], ws[lo, 256:], ws[hi, 256:] = sums
        return 0

    for d in EARLY:
        arrived(d)
    lax.fori_loop(0, 8, functools.partial(point, True, (0,) + EARLY), 0, unroll=True)
    for d in LATE:
        arrived(d)
    lax.fori_loop(0, 8, functools.partial(point, False, LATE), 0, unroll=True)

    parts = []
    for t in range(2):
        lanes = slice(256 * t, 256 * t + 256)
        around = transform([(ws[8 * m : 8 * m + 8, lanes], ws[64 + 8 * m : 72 + 8 * m, lanes]) for m in range(8)], 1.0)
        turns = [(vwdt[0, r : r + 1], vwdt[1, r : r + 1]) for r in range(8)]
        parts += [re * c - im * s for (re, im), (c, s) in zip(around, turns)]
        parts += [im * c + re * s for (re, im), (c, s) in zip(around, turns)]
    y = split(jnp.concatenate(parts, axis=0))
    far_half = 1 - lax.div(z, 4)
    halves = (far_half, 1 - far_half)
    sign = sign[:128]

    mine = mp * 16 + my_u
    for o, a in enumerate(halves):
        back = dot3((mdt[a, 0], mdt[a, 1]), y, True)
        for t in range(2):
            lanes = slice(128 * t, 128 * t + 128)
            snd5[o, 128 * t : 128 * t + 128] = back[:128, lanes] - sign * swap(back[128:, lanes])
        spread(y_peers, snd5.at[o], buf5.at[o], mine, my_row, 8, s5.at[o], r5.at[o], 1)

    for o, a in enumerate(halves):
        landed(buf5.at[o], r5.at[o])
        for i in range(16):
            b = 8 * i
            snd6[o, pl.ds(i, 8, stride=16)] = buf5[o, b : b + 8] + buf5[o, 128 + b : 136 + b]
        own = lax.rem(mz, 8)
        for d in (4, 3, 5, 2, 6, 1, 7, 0):
            n = turn(own, d, 8)
            if d or o == 0:
                pltpu.make_async_remote_copy(
                    tile(snd6.at[o], n, 16), tile(buf6, mz, 16), s6, r6,
                    device_id={"slab": (a * 4 + lax.div(n, 2)) * 4 + mh * 2 + lax.rem(n, 2)},
                    device_id_type=MESH).start()
            else:
                pltpu.make_async_copy(tile(snd6.at[o], n, 16), tile(buf6, mz, 16), r6).start()
    landed(buf1.at[: 8 * (NC - 1)], s1)
    landed(buf2.at[: 16 * (NZ - 1)], s2)
    landed(buf3.at[: 16 * (NY - 1)], s3)
    for o in range(2):
        landed(buf5.at[o, : 8 * (NY - 1)], s5.at[o])
    landed(prm.at[:7], sp)
    landed(vrecv, sv)
    landed(buf6, r6)
    p0, p1 = buf6[pl.ds(0, 128, stride=2)], buf6[pl.ds(1, 128, stride=2)]
    re, im = jnp.where(low, p0, swap(p1)), jnp.where(low, swap(p0), p1)
    z = dot3(split(jnp.concatenate([re.T, im.T], axis=1)), both(mb), False)
    re, im = z[:, :128], z[:, 128:]
    z = jnp.concatenate([re * vwb[0] + im * vwb[1], im * vwb[0] - re * vwb[1]], axis=0)
    snd7[...] = dot3(both(mat), split(z), False)

    spread(chan_peers, snd7, buf7, chan, chan, 8, s7, r7)
    landed(buf7, r7)
    landed(buf6.at[: 16 * (NZ - 1)], s6)
    landed(buf7.at[: 8 * (NC - 1)], s7)
    out[...] = buf7[...]


def local(taylor_models, gridded_vis, uv_weight, freq_ratio, robust_scale):
    tabs = [jnp.asarray(x) for x in tables()]
    any_space = pl.BlockSpec(memory_space=pltpu.HBM)
    v = pltpu.VMEM
    dma = pltpu.SemaphoreType.DMA
    scratch = (
        [pltpu.SMEM((1,), F32), pltpu.SMEM((1,), F32), v((128, 128), F32), v((2, 64, PIX), BF16), v((64, PIX), BF16)]
        + [v(x.shape, F32) for x in tabs]
        + [v((2, *s), BF16) for s in
           ((128, 256), (256, 256), (512, 256), (2, 256, 256), (128, 128))]
        + [v((2, 128, 256), F32)]
        + [v(s, F32) for s in
           ((128, 128), (256, 128), (256, 128), (256, 128), (512, 128), (128, 512), (128, 512),
            (2, 256, 128), (2, 256, 128), (2, 128, 128), (256, 128), (128, 128), (128, 128))]
        + [v((8, 3, 8, PIX), F32), v((7, 3, 8, PIX), F32), v((8, 8, 128), F32)]
        + [dma((12,)), dma, dma, dma, dma((2,)), dma, dma, dma, dma, dma, dma, dma, dma((2,)), dma, dma, dma((8,)), dma((8,))] + [pltpu.SemaphoreType.REGULAR]
    )
    out = pl.pallas_call(
        kernel,
        out_shape=pltpu.VMEM((128, 128), F32),
        in_specs=[any_space] * 12,
        out_specs=pl.BlockSpec(memory_space=pltpu.VMEM),
        scratch_shapes=scratch,
        compiler_params=pltpu.CompilerParams(
            collective_id=0, has_side_effects=True, vmem_limit_bytes=66_000_000),
    )(freq_ratio, robust_scale, taylor_models.reshape(128, 128), gridded_vis[0], uv_weight[0], *tabs)
    return out.reshape(2, 64, 128)


def solution(mesh):
    placed = (
        P(None, "slab", "chan"),
        P("chan", None, "slab", None),
        P("chan", "slab", None),
        P("chan"),
        P("chan"),
    )
    return jax.shard_map(
        local, mesh=mesh, in_specs=placed, out_specs=P(None, "slab", "chan"), check_vma=False
    )
```
